32 devices in a mesh: ctx: 8 (over z, x), inner: 4 (over y, core).
Axes of the slice: x: 2, y: 2, z: 4, core: 2. Of those that a mesh axis runs over, the one named last changes fastest.
Arguments:
- queries: bfloat16 [4096, 512], P(('ctx', 'inner')), may hold values from -8 to 8
- keys: bfloat16 [4096, 512], P(('ctx', 'inner')), may hold values from -6 to 6
- values: bfloat16 [4096, 512], P(('ctx', 'inner')), may hold values from -6 to 6
- w_proj: bfloat16 [8, 64, 256], replicated, may hold values from -1.5 to 1.5
- ln_gain: float32 [2, 64], replicated, may hold values from 0.1 to 1.9
- ln_bias: float32 [2, 64], replicated, may hold values from -3 to 3
- cotangent: bfloat16 [4096, 512], P(('ctx', 'inner')), may hold values from -6 to 6
Outputs:
- attended: bfloat16 [4096, 512], P(('ctx', 'inner'))
- grad_queries: bfloat16 [4096, 512], P(('ctx', 'inner'))
- grad_keys: bfloat16 [4096, 512], P(('ctx', 'inner'))
- grad_values: bfloat16 [4096, 512], P(('ctx', 'inner'))
- grad_proj: float32 [8, 8, 64, 256], P('ctx', None, None, 'inner')
- grad_norm: float32 [4, 64], replicated
The draws below stay inside these ranges and needn't reach their ends.
All inputs are finite; a program needn't handle non-finite values.
Results may differ from the reference program's by a relative error of at most 0.012.
Values may be sent and summed in bfloat16 or wider, within the bound.
No kernel may reach another device: no remote copies, remote signals or barrier semaphores. Data moves between devices by JAX's collectives and lax.ppermute only.
A program may use at most 64 MiB of HBM per device.

```python
import math
import jax
import jax.numpy as jnp
from jax import lax

HEADS = 8
DH = 64
LANDMARKS = 256
WIN = 128
TOKENS = 4096
FEATURES = 512
N_CTX = 8


def draw_keys(key, part):
    result = jnp.clip(jax.random.normal(jax.random.fold_in(key, 11), (TOKENS, HEADS * DH), jnp.float32), -6.0, 6.0)
    return result.astype(jnp.bfloat16)


def draw_queries(key, part):
    result = jnp.clip(jax.random.normal(jax.random.fold_in(key, 23), (TOKENS, HEADS * DH), jnp.float32), -6.0, 6.0)
    return result.astype(jnp.bfloat16)


def draw_w_proj(key, part):
    result = jnp.clip(0.375 * jax.random.normal(jax.random.fold_in(key, 37), (HEADS, DH, LANDMARKS), jnp.float32), -1.5, 1.5)
    return result.astype(jnp.bfloat16)


def shard_levels(rng, dims, shards, low, high):
    factor_of, own = 1.0, jax.random.fold_in(rng, 6)
    for dim, parts in shards:
        draws = jnp.exp(jax.random.uniform(jax.random.fold_in(own, dim), (parts,), jnp.float32, low / len(shards), high / len(shards)))
        factor_of = factor_of * jnp.repeat(draws, dims[dim] // parts).reshape([-1 if axis == dim else 1 for axis in range(len(dims))])
    return factor_of


def scatter_about(stream_key, dims, deviation, limit, pieces=(), held_as=jnp.bfloat16):
    values = deviation * jax.random.normal(stream_key, dims, jnp.float32)
    if pieces:
        values = values * shard_levels(stream_key, dims, pieces, -0.22, 0.18)
    return jnp.clip(values, -limit, limit).astype(held_as)


def setup_inputs(seed: int = 0) -> dict:
    streams_of = jax.random.split(jax.random.key(seed), 8)
    queries = draw_queries(jax.random.fold_in(streams_of[7], 71), 0)
    keys = draw_keys(jax.random.fold_in(streams_of[7], 71), 0)
    values = scatter_about(streams_of[2], (TOKENS, FEATURES), 1.0, 6.0, ((0, 32),))
    w_proj = draw_w_proj(jax.random.fold_in(streams_of[7], 71), 0)
    ln_gain = jnp.clip(1.0 + 0.18 * jax.random.normal(streams_of[4], (2, DH), jnp.float32), 0.1, 1.9)
    ln_bias = scatter_about(streams_of[5], (2, DH), 0.5, 3.0, (), jnp.float32)
    cotangent = scatter_about(streams_of[6], (TOKENS, FEATURES), 1.0, 6.0, ((0, 32),))
    return dict(queries=queries, keys=keys, values=values, w_proj=w_proj, ln_gain=ln_gain, ln_bias=ln_bias, cotangent=cotangent)


def rounded(values_in):
    narrowed = lax.optimization_barrier(values_in.astype(jnp.bfloat16))
    return narrowed.astype(jnp.float32)

def normalise(landmark, gain_row, bias_row):
    average = lax.optimization_barrier(jnp.mean(landmark, axis=-1, keepdims=True))
    centred = landmark - average
    variance = lax.optimization_barrier(jnp.mean(centred * centred, axis=-1, keepdims=True))
    inverse = 1.0 / jnp.sqrt(variance + 1e-05)
    normed = centred * inverse
    return (normed, inverse, normed * gain_row + bias_row)

def norm_backward(grad_out, normed, inverse, gain_row):
    grad_normed = grad_out * gain_row
    first_mean = lax.optimization_barrier(jnp.mean(grad_normed, axis=-1, keepdims=True))
    second_mean = lax.optimization_barrier(jnp.mean(grad_normed * normed, axis=-1, keepdims=True))
    grad_in = inverse * (grad_normed - first_mean - normed * second_mean)
    return (grad_in, lax.optimization_barrier(jnp.sum(grad_out * normed, axis=(0, 1))), lax.optimization_barrier(jnp.sum(grad_out, axis=(0, 1))))

def reference(queries, keys, values, w_proj, ln_gain, ln_bias, cotangent):
    segments = TOKENS // WIN
    per_group = segments // N_CTX
    edge = 3 * WIN
    score_scale = 1.0 / math.sqrt(DH)
    query_seg = queries.reshape(segments, WIN, HEADS, DH)
    key_seg = keys.reshape(segments, WIN, HEADS, DH)
    value_seg = values.reshape(segments, WIN, HEADS, DH)
    grad_seg = cotangent.reshape(segments, WIN, HEADS, DH)
    w_full = w_proj.astype(jnp.float32)
    pad_spec = ((1, 1), (0, 0), (0, 0), (0, 0))
    key_pad = jnp.pad(key_seg, pad_spec)
    value_pad = jnp.pad(value_seg, pad_spec)
    query_pad = jnp.pad(query_seg, pad_spec)
    grad_pad = jnp.pad(grad_seg, pad_spec)

    def seg_logits(block):
        return jnp.einsum('thd,hdr->htr', block.astype(jnp.float32), w_full)

    def peak_step(carry, block):
        return (jnp.maximum(carry, lax.optimization_barrier(jnp.max(seg_logits(block), axis=1))), None)
    column_peak = lax.scan(peak_step, jnp.full((HEADS, LANDMARKS), -1e+30, jnp.float32), key_seg)[0]

    def total_step(carry, blocks):
        exponent = jnp.exp(seg_logits(blocks[0]) - column_peak[:, None, :])
        narrowed = rounded(exponent)
        key_part = jnp.einsum('htr,thd->hrd', narrowed, blocks[0].astype(jnp.float32))
        value_part = jnp.einsum('htr,thd->hrd', narrowed, blocks[1].astype(jnp.float32))
        return ((carry[0] + lax.optimization_barrier(jnp.sum(exponent, axis=1)), carry[1] + key_part, carry[2] + value_part), None)
    start = (jnp.zeros((HEADS, LANDMARKS), jnp.float32), jnp.zeros((HEADS, LANDMARKS, DH), jnp.float32), jnp.zeros((HEADS, LANDMARKS, DH), jnp.float32))
    sums = lax.scan(total_step, start, (key_seg, value_seg))[0]
    column_total = sums[0]
    mean_keys = sums[1] / column_total[..., None]
    mean_values = sums[2] / column_total[..., None]
    normed_keys, inverse_keys, land_keys = normalise(mean_keys, ln_gain[0], ln_bias[0])
    normed_values, inverse_values, land_values = normalise(mean_values, ln_gain[1], ln_bias[1])
    land_key_r = rounded(land_keys).transpose(1, 0, 2)
    land_value_r = rounded(land_values).transpose(1, 0, 2)

    def attend_step(carry, seg_index):
        query_block = query_seg[seg_index].astype(jnp.float32)
        grad_block = grad_seg[seg_index].astype(jnp.float32)
        window_keys = lax.dynamic_slice_in_dim(key_pad, seg_index, 3, 0).reshape(edge, HEADS, DH).astype(jnp.float32)
        window_values = lax.dynamic_slice_in_dim(value_pad, seg_index, 3, 0).reshape(edge, HEADS, DH).astype(jnp.float32)
        all_keys = jnp.concatenate([window_keys, land_key_r], axis=0)
        all_values = jnp.concatenate([window_values, land_value_r], axis=0)
        neighbour = seg_index - 1 + jnp.arange(edge, dtype=jnp.int32) // WIN
        usable = jnp.concatenate([(neighbour >= 0) & (neighbour < segments), jnp.ones((LANDMARKS,), dtype=bool)])
        scores = jnp.einsum('qhd,khd->hqk', query_block, all_keys) * score_scale
        scores = jnp.where(usable[None, None, :], scores, -1e+30)
        row_peak = lax.optimization_barrier(jnp.max(scores, axis=-1))
        log_total = row_peak + jnp.log(lax.optimization_barrier(jnp.sum(jnp.exp(scores - row_peak[..., None]), axis=-1)))
        probs = jnp.exp(scores - log_total[..., None])
        narrowed = rounded(probs)
        output = jnp.einsum('hqk,khd->qhd', narrowed, all_values)
        delta = jnp.einsum('qhd,qhd->hq', grad_block, output)
        grad_probs = jnp.einsum('qhd,khd->hqk', grad_block, all_values)
        grad_scores = rounded(probs * (grad_probs - delta[..., None]))
        grad_query = jnp.einsum('hqk,khd->qhd', grad_scores, all_keys) * score_scale
        land_key_grad = carry[0] + jnp.einsum('hqr,qhd->hrd', grad_scores[..., edge:], query_block) * score_scale
        land_value_grad = carry[1] + jnp.einsum('hqr,qhd->hrd', narrowed[..., edge:], grad_block)
        results = (output.astype(jnp.bfloat16), grad_query.astype(jnp.bfloat16), log_total, delta)
        return ((land_key_grad, land_value_grad), results)
    land_start = (jnp.zeros((HEADS, LANDMARKS, DH), jnp.float32), jnp.zeros((HEADS, LANDMARKS, DH), jnp.float32))
    land_grads, forward_rows = lax.scan(attend_step, land_start, jnp.arange(segments, dtype=jnp.int32))
    attended = forward_rows[0].reshape(TOKENS, FEATURES)
    grad_queries = forward_rows[1].reshape(TOKENS, FEATURES)
    lse_pad = jnp.pad(forward_rows[2], ((1, 1), (0, 0), (0, 0)))
    delta_pad = jnp.pad(forward_rows[3], ((1, 1), (0, 0), (0, 0)))
    grad_mean_keys, gain_key_grad, bias_key_grad = norm_backward(land_grads[0], normed_keys, inverse_keys, ln_gain[0])
    grad_mean_values, gain_value_grad, bias_value_grad = norm_backward(land_grads[1], normed_values, inverse_values, ln_gain[1])
    grad_norm = jnp.stack([gain_key_grad, bias_key_grad, gain_value_grad, bias_value_grad])
    grad_key_r = rounded(grad_mean_keys)
    grad_value_r = rounded(grad_mean_values)
    scaled_keys = rounded(grad_mean_keys / column_total[..., None])
    scaled_values = rounded(grad_mean_values / column_total[..., None])

    def weights_of(key_block):
        narrowed = rounded(jnp.exp(seg_logits(key_block) - column_peak[:, None, :]))
        return (narrowed, narrowed / column_total[:, None, :])

    def proj_grad(key_block, value_block):
        first = jnp.einsum('thd,hrd->htr', key_block.astype(jnp.float32), grad_key_r)
        return first + jnp.einsum('thd,hrd->htr', value_block.astype(jnp.float32), grad_value_r)

    def column_step(carry, blocks):
        weights = weights_of(blocks[0])[1]
        return (carry + lax.optimization_barrier(jnp.sum(weights * proj_grad(blocks[0], blocks[1]), axis=1)), None)
    column_sum = lax.scan(column_step, jnp.zeros((HEADS, LANDMARKS), jnp.float32), (key_seg, value_seg))[0]

    def key_step(carry, seg_index):
        key_block = key_seg[seg_index].astype(jnp.float32)
        value_block = value_seg[seg_index].astype(jnp.float32)
        narrowed, weights = weights_of(key_seg[seg_index])
        grad_logit = rounded(weights * (proj_grad(key_seg[seg_index], value_seg[seg_index]) - column_sum[:, None, :]))
        grad_key = jnp.einsum('htr,hrd->thd', narrowed, scaled_keys) + jnp.einsum('htr,hdr->thd', grad_logit, w_full)
        grad_value = jnp.einsum('htr,hrd->thd', narrowed, scaled_values)
        new_carry = carry + jnp.einsum('thd,htr->hdr', key_block, grad_logit)
        for offset in (0, 1, 2):
            source = seg_index + offset
            real_seg = source - 1
            usable = (real_seg >= 0) & (real_seg < segments)
            query_block = query_pad[source].astype(jnp.float32)
            grad_block = grad_pad[source].astype(jnp.float32)
            cross = jnp.einsum('qhd,khd->hqk', query_block, key_block) * score_scale
            probs = jnp.where(usable, jnp.exp(cross - lse_pad[source][..., None]), 0.0)
            grad_probs = jnp.einsum('qhd,khd->hqk', grad_block, value_block)
            grad_scores = rounded(probs * (grad_probs - delta_pad[source][..., None]))
            grad_key = grad_key + jnp.einsum('hqk,qhd->khd', grad_scores, query_block) * score_scale
            grad_value = grad_value + jnp.einsum('hqk,qhd->khd', rounded(probs), grad_block)
        return (new_carry, (grad_key.astype(jnp.bfloat16), grad_value.astype(jnp.bfloat16)))

    def group_step(group):
        indices = group * per_group + jnp.arange(per_group, dtype=jnp.int32)
        return lax.scan(key_step, jnp.zeros((HEADS, DH, LANDMARKS), jnp.float32), indices)
    grad_proj, key_rows = lax.map(group_step, jnp.arange(N_CTX, dtype=jnp.int32))
    grad_keys = key_rows[0].reshape(TOKENS, FEATURES)
    grad_values = key_rows[1].reshape(TOKENS, FEATURES)
    return (attended, grad_queries, grad_keys, grad_values, grad_proj, grad_norm)
```

```python
import functools
import math

import jax
import jax.numpy as jnp
import numpy as np
from jax import lax
from jax.experimental import pallas as pl
from jax.experimental.pallas import tpu as pltpu
from jax.sharding import Mesh
from jax.sharding import PartitionSpec as P

WIN = 128
EXTRA = 16
EPS = 1e-05
NEG = -1e30
BF = jnp.bfloat16
F32 = jnp.float32

NN = (((1,), (0,)), ((), ()))
NT = (((1,), (1,)), ((), ()))
SEQ = ("seq", "half")
HEAD = ("sub", "part")


def dot(a, b, dims=NN):
    return lax.dot_general(a, b, dims, preferred_element_type=F32)


def lanes(shape):
    return lax.broadcasted_iota(jnp.int32, shape, 1)


def rows(shape):
    return lax.broadcasted_iota(jnp.int32, shape, 0)


def pack_kernel(q_ref, k_ref, v_ref, g_ref, o_ref):
    heads, _, width = o_ref.shape
    dh = width // 4
    for h in range(heads):
        cols = slice(h * dh, (h + 1) * dh)
        for slot, ref in enumerate((k_ref, v_ref, q_ref, g_ref)):
            o_ref[h, :, slot * dh : (slot + 1) * dh] = ref[:, cols]


def split_rows(total_rows, width, pieces):
    r = rows((total_rows, width))
    out = jnp.zeros((total_rows, width), F32)
    for index, piece in enumerate(pieces):
        out = jnp.where(r == index, piece, out)
    return out.astype(BF)


def bf_pieces(x, count):
    out = []
    for _ in range(count):
        piece = x.astype(BF).astype(F32)
        out.append(piece)
        x = x - piece
    return out


def widen_proj(w):
    return jnp.concatenate([w, jnp.zeros_like(w)], axis=0)


def local_sums_kernel(h_ref, x_ref, w_ref, mid_ref, *out_refs):
    del h_ref
    expo_ref = out_refs[-1]
    pair = x_ref.shape[1] // 2
    kv = x_ref[:, :pair]
    logits = dot(kv, widen_proj(w_ref[0]))
    peak = jnp.max(logits, axis=0, keepdims=True)
    expo = jnp.exp(logits - peak)
    total = jnp.sum(expo, axis=0, keepdims=True)
    expo_b = expo.astype(BF)
    expo_ref[...] = expo_b
    sums = dot(kv.T, expo_b).astype(BF)
    marks = sums.shape[1]
    tail = split_rows(EXTRA, marks, bf_pieces(peak, 3) + bf_pieces(total, 2))
    targets = [(mid_ref, None)]
    if len(out_refs) == 3:
        count = x_ref.shape[0]
        targets += [(out_refs[0], kv[count - WIN :]), (out_refs[1], kv[:WIN])]
    for ref, halo in targets:
        ref[:pair, :marks] = sums
        ref[pair:, :marks] = tail
        if halo is not None:
            ref[:pair, marks:] = halo
            ref[pair:, marks:] = jnp.zeros((EXTRA, pair), BF)


def collect(own_ref, recv_refs, stack_ref, index, marks):
    count = len(recv_refs) + 1
    stack_ref[index] = own_ref[...]
    for shift, ref in enumerate(recv_refs, start=1):
        stack_ref[lax.rem(index + (count - shift), count)] = ref[:, :marks]


def attention_kernel(*refs, ring, scale):
    if ring > 0:
        z_ref, x_ref, own_ref, *recv = refs[:3 + ring]
        gain_ref, bias_ref = refs[3 + ring : 5 + ring]
        rest = refs[5 + ring :]
    else:
        z_ref, x_ref, stack_ref, prev_ref, next_ref, gain_ref, bias_ref = refs[:7]
        rest = refs[7:]
    count, width = x_ref.shape
    pair = width // 2
    dh = pair // 2
    segments = count // WIN
    if ring > 0:
        od_ref, dkvt_ref, mid_ref, plus_ref, minus_ref, stats_ref, kvp_ref, acc_ref, stack_ref = rest
    else:
        od_ref, dkvt_ref, mid_ref, plus_ref, minus_ref, stats_ref, kvp_ref, acc_ref = rest
    marks = mid_ref.shape[1]
    z = z_ref[0]
    last = z_ref[1] - 1
    if ring > 0:
        collect(own_ref, recv, stack_ref, z, marks)
        prev_halo = recv[0][:pair, marks:]
        next_halo = recv[-1][:pair, marks:]
    else:
        prev_halo = prev_ref[...]
        next_halo = next_ref[...]
    groups = stack_ref.shape[0]
    kvp_ref[:WIN] = prev_halo
    kvp_ref[WIN : WIN + count] = x_ref[:, :pair]
    kvp_ref[WIN + count :] = next_halo

    peaks, totals = [], []
    for j in range(groups):
        tail = stack_ref[j, pair:, :].astype(F32)
        peaks.append(tail[0:1] + tail[1:2] + tail[2:3])
        totals.append(tail[3:4] + tail[4:5])
    peak = functools.reduce(jnp.maximum, peaks)
    total = jnp.zeros_like(peak)
    sums = jnp.zeros((pair, marks), F32)
    for j in range(groups):
        factor = jnp.exp(peaks[j] - peak)
        total = total + factor * totals[j]
        sums = sums + factor * stack_ref[j, :pair, :].astype(F32)
    mean = sums / total
    normed, inverse = [], []
    for half in range(2):
        block = mean[half * dh : (half + 1) * dh]
        centred = block - jnp.mean(block, axis=0, keepdims=True)
        variance = jnp.mean(centred * centred, axis=0, keepdims=True)
        inv = 1.0 / jnp.sqrt(variance + EPS)
        normed.append(centred * inv)
        inverse.append(inv)
    normed = jnp.concatenate(normed, axis=0)
    land_f = normed * gain_ref[...] + bias_ref[...]
    land_t = land_f.astype(BF)
    land = land_f.T.astype(BF)
    stack_own = stack_ref[z, pair:, :].astype(F32)
    own_peak = stack_own[0:1] + stack_own[1:2] + stack_own[2:3]
    factor = jnp.exp(own_peak - peak) / total
    stats_ref[:pair] = normed
    stats_ref[pair : 2 * pair] = mean
    r8 = rows((8, marks))
    stats_ref[2 * pair :] = jnp.where(r8 == 0, inverse[0], jnp.where(r8 == 1, inverse[1], factor))

    acc_ref[...] = jnp.zeros(acc_ref.shape, F32)
    land_grad = jnp.zeros((pair, marks), F32)
    low = lanes((WIN, pair)) < dh
    zero_b = jnp.zeros((WIN, pair), BF)
    for s in range(segments):
        qg = x_ref[s * WIN : (s + 1) * WIN, pair:]
        q0 = jnp.where(low, (qg.astype(F32) * scale).astype(BF), zero_b)
        g0 = jnp.where(low, zero_b, qg)
        a = jnp.concatenate([q0, g0], axis=0)
        kvw = kvp_ref[s * WIN : (s + 3) * WIN]
        sw = dot(a, kvw, NT)
        sl = dot(a, land_t)
        s_w, gp_w = sw[:WIN], sw[WIN:]
        s_l, gp_l = sl[:WIN], sl[WIN:]
        if s == 0:
            s_w = jnp.where((lanes(s_w.shape) < WIN) & (z == 0), NEG, s_w)
        if s == segments - 1:
            s_w = jnp.where((lanes(s_w.shape) >= 2 * WIN) & (z == last), NEG, s_w)
        top = jnp.maximum(
            jnp.max(s_w, axis=1, keepdims=True), jnp.max(s_l, axis=1, keepdims=True)
        )
        e_w = jnp.exp(s_w - top)
        e_l = jnp.exp(s_l - top)
        inv = 1.0 / (
            jnp.sum(e_w, axis=1, keepdims=True) + jnp.sum(e_l, axis=1, keepdims=True)
        )
        p_w = e_w * inv
        p_l = e_l * inv
        pb_w = p_w.astype(BF)
        pb_l = p_l.astype(BF)
        delta = jnp.sum(pb_w.astype(F32) * gp_w, axis=1, keepdims=True) + jnp.sum(
            pb_l.astype(F32) * gp_l, axis=1, keepdims=True
        )
        b_w = jnp.concatenate([(p_w * (gp_w - delta)).astype(BF), pb_w], axis=0)
        b_l = jnp.concatenate([(p_l * (gp_l - delta)).astype(BF), pb_l], axis=0)
        od = dot(b_w, kvw) + dot(b_l, land)
        od_ref[s * WIN : (s + 1) * WIN] = jnp.where(low, od[:WIN] * scale, od[WIN:]).astype(BF)
        at = a.T
        acc_ref[:, s * WIN : (s + 3) * WIN] += dot(at, b_w)
        land_grad = land_grad + dot(at, b_l)
    dkvt_ref[...] = acc_ref[:, WIN : WIN + count]
    land_b = land_grad.astype(BF)
    mid_ref[...] = land_b
    if ring > 0:
        plus_ref[:, :marks] = land_b
        plus_ref[:, marks:] = acc_ref[:, WIN + count :].astype(BF)
        minus_ref[:, :marks] = land_b
        minus_ref[:, marks:] = acc_ref[:, :WIN].astype(BF)
    else:
        plus_ref[...] = acc_ref[:, WIN + count :].astype(BF)
        minus_ref[...] = acc_ref[:, :WIN].astype(BF)


def final_kernel(*refs, ring, sub, parts, tiled):
    if ring > 0:
        z_ref, own_ref, *recv = refs[: 2 + ring]
        rest = refs[2 + ring :]
    else:
        z_ref, stack_ref, prev_ref, next_ref = refs[:4]
        rest = refs[4:]
    x_ref, w_ref, gain_ref, expo_ref, od_ref, dkvt_ref, stats_ref = rest[:7]
    outs = rest[7:]
    send_ref = outs[0]
    count, width = x_ref.shape
    pair = width // 2
    dh = pair // 2
    marks = expo_ref.shape[1]
    z = z_ref[0]
    last = z_ref[1] - 1
    if ring > 0:
        stack_ref = outs[-1]
        collect(own_ref, recv, stack_ref, z, marks)
        from_prev = recv[0][:, marks:]
        from_next = recv[-1][:, marks:]
    else:
        from_prev = prev_ref[...]
        from_next = next_ref[...]
    from_prev = jnp.where(z == 0, 0.0, from_prev.astype(F32))
    from_next = jnp.where(z == last, 0.0, from_next.astype(F32))
    grad = stack_ref[0].astype(F32)
    for j in range(1, stack_ref.shape[0]):
        grad = grad + stack_ref[j].astype(F32)
    normed = stats_ref[:pair]
    mean = stats_ref[pair : 2 * pair]
    factor = stats_ref[2 * pair + 2 : 2 * pair + 3]
    gained = grad * gain_ref[...]
    blocks = []
    for half in range(2):
        part = slice(half * dh, (half + 1) * dh)
        g = gained[part]
        first = jnp.mean(g, axis=0, keepdims=True)
        second = jnp.mean(g * normed[part], axis=0, keepdims=True)
        inv = stats_ref[2 * pair + half : 2 * pair + half + 1]
        blocks.append(inv * (g - first - normed[part] * second))
    grad_mean = jnp.concatenate(blocks, axis=0)
    grad_b = grad_mean.astype(BF)
    column = jnp.sum(grad_b.astype(F32) * mean, axis=0, keepdims=True)
    scaled = (grad_mean * factor).astype(BF)

    gain_sum = jnp.sum(grad * normed, axis=1, keepdims=True)
    bias_sum = jnp.sum(grad, axis=1, keepdims=True)
    lane = lanes((pair, pair))
    square = jnp.where(lane == 0, gain_sum, jnp.where(lane == 1, bias_sum, 0.0)).T
    norm_hi = square[:8].astype(BF)
    norm_lo = (square[:8] - norm_hi.astype(F32)).astype(BF)
    norm_rows = jnp.concatenate(
        [
            jnp.concatenate([norm_hi.astype(F32), norm_lo.astype(F32)], axis=1),
            jnp.zeros((8, width), F32),
        ],
        axis=0,
    ).astype(BF)

    kv = x_ref[:, :pair]
    wide = widen_proj(w_ref[0])
    expo_b = expo_ref[...]
    weights = expo_b.astype(F32) * factor
    grad_logit = (weights * (dot(kv, grad_b) - column)).astype(BF)
    land = dot(expo_b, scaled, NT) + dot(grad_logit, wide, NT)
    window = dkvt_ref[...].T
    dests, out_rows, _ = send_ref.shape
    step = count // dests
    dkv = land + window
    head_fix = from_prev.T
    tail_fix = from_next.T
    for d in range(dests):
        span = slice(d * step, (d + 1) * step)
        block = dkv[span]
        fix_top = head_fix if d == 0 else None
        fix_end = tail_fix if d == dests - 1 else None
        for at in range(0, step, WIN):
            piece = block[at : at + WIN]
            if fix_top is not None and at == 0:
                piece = piece + fix_top
            if fix_end is not None and at + WIN == step:
                piece = piece + fix_end
            send_ref[d, at : at + WIN, :pair] = piece.astype(BF)
        send_ref[d, :step, pair:] = od_ref[span]
        send_ref[d, step : step + 16] = norm_rows
    kvt = kv.T
    group = count // sub
    for sb in range(sub):
        span = slice(sb * group, (sb + 1) * group)
        proj = dot(kvt[:, span], grad_logit[span])[:dh]
        if tiled:
            wide_part = marks // parts
            quarter = dh // 4
            for i in range(parts):
                tile = proj[:, i * wide_part : (i + 1) * wide_part].astype(BF)
                for k in range(4):
                    send_ref[
                        sb * parts + i, step + 16 :, k * dh : (k + 1) * dh
                    ] = tile[k * quarter : (k + 1) * quarter]
        else:
            outs[1][...] = proj


def unpack_kernel(r_ref, att_ref, dq_ref, dk_ref, dv_ref, norm_ref, *proj_refs):
    heads, _, width = r_ref.shape
    dh = width // 4
    pair = 2 * dh
    step = att_ref.shape[0]
    for h in range(heads):
        cols = slice(h * dh, (h + 1) * dh)
        for slot, ref in enumerate((dk_ref, dv_ref, dq_ref, att_ref)):
            ref[:, cols] = r_ref[h, :step, slot * dh : (slot + 1) * dh]
    norm = jnp.zeros((8, pair), F32)
    for h in range(heads):
        block = r_ref[h, step : step + 16, :].astype(F32)[:8]
        norm = norm + (block[:, :pair] + block[:, pair:])
    norm_ref[0:1] = norm[0:1, :dh]
    norm_ref[1:2] = norm[1:2, :dh]
    norm_ref[2:3] = norm[0:1, dh:]
    norm_ref[3:4] = norm[1:2, dh:]
    if proj_refs:
        proj_ref = proj_refs[0]
        quarter = dh // 4
        for h in range(heads):
            for k in range(4):
                proj_ref[0, h, k * quarter : (k + 1) * quarter] = r_ref[
                    h, step + 16 :, k * dh : (k + 1) * dh
                ].astype(F32)


def shape_of(shape, dtype):
    return jax.ShapeDtypeStruct(shape, dtype)


VM = pl.BlockSpec(memory_space=pltpu.VMEM)
SM = pl.BlockSpec(memory_space=pltpu.SMEM)


def call(kernel, out_shape, args, specs, name, scratch=()):
    return pl.pallas_call(
        kernel,
        out_shape=out_shape,
        in_specs=specs,
        out_specs=jax.tree.map(lambda _: VM, out_shape),
        scratch_shapes=scratch,
        name=name,
    )(*args)


def per_device(queries, keys, values, w_proj, ln_gain, ln_bias, cotangent):
    tokens_dev, features = queries.shape
    heads, dh, marks = w_proj.shape
    pair = 2 * dh
    width = 4 * dh
    count = tokens_dev * heads
    scale = 1.0 / math.sqrt(dh)
    seqs = lax.axis_size(SEQ)
    sub = lax.axis_size("sub")
    parts = lax.axis_size("part")
    halves = lax.axis_size("half")
    head = lax.axis_index(HEAD).astype(jnp.int32)
    z = lax.axis_index(SEQ).astype(jnp.int32)
    place = jnp.stack([z, jnp.int32(seqs)])
    ring = seqs - 1 if 3 <= seqs <= 8 else 0
    wide_part = marks // parts
    tiled = halves == 1 and wide_part == dh and dh % 64 == 0

    packed = call(
        pack_kernel,
        shape_of((heads, tokens_dev, width), BF),
        (queries, keys, values, cotangent),
        [VM] * 4,
        "pack",
    )
    x = lax.all_to_all(packed, HEAD, 0, 0, tiled=True).reshape(count, width)
    w_head = lax.dynamic_slice_in_dim(w_proj, head, 1, axis=0)

    rows_out = pair + EXTRA
    out_shape = [shape_of((rows_out, marks), BF)]
    if ring:
        out_shape += [shape_of((rows_out, marks + pair), BF)] * 2
    out_shape.append(shape_of((count, marks), BF))
    mid, *halo_outs, expo = call(
        local_sums_kernel, out_shape, (place, x, w_head), [SM, VM, VM], "local_sums"
    )

    def shifted(block, shift):
        return lax.ppermute(block, SEQ, [(i, (i + shift) % seqs) for i in range(seqs)])

    def forward(block, shift):
        route = [(i, i + shift) for i in range(seqs) if 0 <= i + shift < seqs]
        return lax.ppermute(block, SEQ, route)

    gain = ln_gain.reshape(pair, 1)
    bias = ln_bias.reshape(pair, 1)
    if ring:
        recv = [shifted(halo_outs[0], 1)]
        recv += [shifted(mid, k) for k in range(2, ring)]
        recv += [shifted(halo_outs[1], ring)]
        lands = [mid, *recv]
    else:
        lands = [
            lax.all_gather(mid, SEQ),
            forward(x[count - WIN :, :pair], 1),
            forward(x[:WIN, :pair], -1),
        ]
    halo_wide = marks + pair if ring else pair
    scratch = [pltpu.VMEM((count + 2 * WIN, pair), BF), pltpu.VMEM((pair, count + 2 * WIN), F32)]
    if ring:
        scratch.append(pltpu.VMEM((seqs, rows_out, marks), BF))
    od, dkvt, grad_mid, plus, minus, stats = call(
        functools.partial(attention_kernel, ring=ring, scale=scale),
        [
            shape_of((count, pair), BF),
            shape_of((pair, count), F32),
            shape_of((pair, marks), BF),
            shape_of((pair, halo_wide), BF),
            shape_of((pair, halo_wide), BF),
            shape_of((2 * pair + 8, marks), F32),
        ],
        (place, x, *lands, gain, bias),
        [SM] + [VM] * (len(lands) + 3),
        "attention",
        scratch,
    )
    if ring:
        recv = [shifted(plus, 1)]
        recv += [shifted(grad_mid, k) for k in range(2, ring)]
        recv += [shifted(minus, ring)]
        grads = [grad_mid, *recv]
        scratch = [pltpu.VMEM((seqs, pair, marks), BF)]
    else:
        grads = [lax.all_gather(grad_mid, SEQ), forward(plus, 1), forward(minus, -1)]
        scratch = []
    send_rows = tokens_dev + 16 + (dh // 4 if tiled else 0)
    out_shape = [shape_of((heads, send_rows, width), BF)]
    if not tiled:
        out_shape.append(shape_of((dh, marks), F32))
    send, *proj = call(
        functools.partial(
            final_kernel, ring=ring, sub=sub if tiled else 1, parts=parts, tiled=tiled
        ),
        out_shape,
        (place, *grads, x, w_head, gain, expo, od, dkvt, stats),
        [SM] + [VM] * (len(grads) + 7),
        "landmark_backward",
        scratch,
    )
    back = lax.all_to_all(send, HEAD, 0, 0, tiled=True)
    out_shape = [shape_of((tokens_dev, features), BF)] * 4 + [shape_of((4, dh), F32)]
    if tiled:
        out_shape.append(shape_of((1, heads, dh, wide_part), F32))
    attended, dq, dk, dv, grad_norm, *tiles = call(unpack_kernel, out_shape, (back,), [VM], "unpack")
    if tiled:
        grad_proj = tiles[0]
    else:
        full = lax.all_gather(proj[0], HEAD)
        inner = ("half", "part") if halves > 1 else "part"
        grad_proj = lax.psum_scatter(full, inner, scatter_dimension=2, tiled=True)[None] / parts
    return (attended, dq, dk, dv, grad_proj, grad_norm)


def solution(mesh):
    ctx, inner = mesh.shape["ctx"], mesh.shape["inner"]

    def whole(queries, keys, values, w_proj, ln_gain, ln_bias, cotangent):
        heads = w_proj.shape[0]
        part = min(heads, inner)
        sub = heads // part
        order = np.asarray(mesh.devices).reshape(ctx // sub, sub, inner // part, part)
        split = Mesh(order, ("seq", "sub", "half", "part"))
        every = P(("seq", "sub", "half", "part"), None)
        return jax.shard_map(
            per_device,
            mesh=split,
            in_specs=(every, every, every, P(), P(), P(), every),
            out_specs=(
                every,
                every,
                every,
                every,
                P(("seq", "sub"), None, None, ("half", "part")),
                P(),
            ),
            check_vma=False,
        )(queries, keys, values, w_proj, ln_gain, ln_bias, cotangent)

    return whole
```

```python
import functools
import math

import jax
import jax.numpy as jnp
import numpy as np
from jax import lax
from jax.experimental import pallas as pl
from jax.experimental.pallas import tpu as pltpu
from jax.sharding import Mesh
from jax.sharding import PartitionSpec as P

WIN = 128
EXTRA = 8
EPS = 1e-05
NEG = -1e30
VMEM_LIMIT = 24 * 1024 * 1024
BF = jnp.bfloat16
F32 = jnp.float32

NN = (((1,), (0,)), ((), ()))
NT = (((1,), (1,)), ((), ()))
SEQ = ("seq", "half")
HEAD = ("sub", "part")


def dot(a, b, dims=NN):
    return lax.dot_general(a, b, dims, preferred_element_type=F32)


def lanes(shape):
    return lax.broadcasted_iota(jnp.int32, shape, 1)


def rows(shape):
    return lax.broadcasted_iota(jnp.int32, shape, 0)


def pack_kernel(q_ref, k_ref, v_ref, g_ref, o_ref, buffer_ref, sems):
    heads, _, width = o_ref.shape
    dh = width // 4
    copies = []
    for slot, ref in enumerate((k_ref, v_ref, q_ref, g_ref)):
        copy = pltpu.make_async_copy(ref, buffer_ref.at[slot], sems.at[slot])
        copy.start()
        copies.append(copy)
    for slot, copy in enumerate(copies):
        copy.wait()
        for h in range(heads):
            o_ref[h, :, slot * dh : (slot + 1) * dh] = buffer_ref[slot, :, h * dh : (h + 1) * dh]


def split_rows(total_rows, width, pieces):
    r = rows((total_rows, width))
    out = jnp.zeros((total_rows, width), F32)
    for index, piece in enumerate(pieces):
        out = jnp.where(r == index, piece, out)
    return out.astype(BF)


def bf_pieces(x, count):
    out = []
    for _ in range(count):
        piece = x.astype(BF).astype(F32)
        out.append(piece)
        x = x - piece
    return out


def widen_proj(w):
    return jnp.concatenate([w, jnp.zeros_like(w)], axis=0)


def local_sums_kernel(place_ref, x_ref, w_ref, mid_ref, *out_refs):
    expo_ref = out_refs[-1]
    pair = x_ref.shape[1] // 2
    kv = x_ref[:, :pair]
    logits = dot(kv, widen_proj(w_ref[place_ref[2]]))
    peak = jnp.max(logits, axis=0, keepdims=True)
    expo = jnp.exp(logits - peak)
    total = jnp.sum(expo, axis=0, keepdims=True)
    expo_b = expo.astype(BF)
    expo_ref[...] = expo_b
    sums = dot(kv.T, expo_b).astype(BF)
    marks = sums.shape[1]
    tail = split_rows(EXTRA, marks, bf_pieces(peak, 3) + bf_pieces(total, 2))
    targets = [(mid_ref, None)]
    if len(out_refs) == 3:
        count = x_ref.shape[0]
        targets += [(out_refs[0], kv[count - WIN :]), (out_refs[1], kv[:WIN])]
    for ref, halo in targets:
        ref[:pair, :marks] = sums
        ref[pair:, :marks] = tail
        if halo is not None:
            ref[:pair, marks:] = halo
            ref[pair:, marks:] = jnp.zeros((EXTRA, pair), BF)


def collect(own_ref, recv_refs, stack_ref, index, marks):
    count = len(recv_refs) + 1
    stack_ref[index] = own_ref[...]
    for shift, ref in enumerate(recv_refs, start=1):
        stack_ref[lax.rem(index + (count - shift), count)] = ref[:, :marks]


def as_column(ref):
    row = jnp.concatenate([ref[0:1, :], ref[1:2, :]], axis=1)
    size = row.shape[1]
    return jnp.sum(
        jnp.where(rows((size, size)) == lanes((size, size)), row, 0.0), axis=1, keepdims=True
    )


def spread(x, width):
    return jnp.concatenate([x] * (width // x.shape[1]), axis=1)


def row_max(x):
    return jnp.max(x, axis=1, keepdims=True)


def row_sum(x):
    return jnp.sum(x, axis=1, keepdims=True)


def window_forward_kernel(x_ref, gain_src, bias_src, early_ref, a_ref, at_ref, affine_ref, *, scale):
    count, width = x_ref.shape
    pair = width // 2
    dh = pair // 2
    segments = count // WIN
    low = lanes((WIN, pair)) < dh
    zero_b = jnp.zeros((WIN, pair), BF)
    for slot, src in enumerate((gain_src, bias_src)):
        affine_ref[slot * pair : (slot + 1) * pair] = jnp.broadcast_to(
            as_column(src), (pair, affine_ref.shape[1])
        )
    for s in range(segments):
        qg = x_ref[s * WIN : (s + 1) * WIN, pair:]
        q0 = jnp.where(low, (qg.astype(F32) * scale).astype(BF), zero_b)
        g0 = jnp.where(low, zero_b, qg)
        a = jnp.concatenate([q0, g0], axis=0)
        a_ref[2 * s * WIN : 2 * (s + 1) * WIN] = a
        at_ref[s * pair : (s + 1) * pair] = a.T
        kvw = x_ref[max(s - 1, 0) * WIN : min(s + 2, segments) * WIN, :pair]
        sw = dot(a, kvw, NT)
        scores, grads = sw[:WIN], sw[WIN:]
        top = row_max(scores)
        expo = jnp.exp(scores - top)
        expo_b = expo.astype(BF)
        out = dot(expo_b, kvw)
        part = row_sum(expo_b.astype(F32) * grads)
        span = slice(s * WIN, (s + 1) * WIN)
        early_ref[span, :pair] = out
        for slot, stat in enumerate((top, row_sum(expo), part), start=1):
            early_ref[span, slot * pair : (slot + 1) * pair] = jnp.broadcast_to(stat, out.shape)


def landmark_forward_kernel(*refs, ring):
    lands = ring + 1 if ring else 3
    place_ref, early_ref, a_ref, at_ref = refs[:4]
    land_refs = refs[4 : 4 + lands]
    affine_ref = refs[4 + lands]
    outs = refs[5 + lands :]
    late_ref, rows_ref, mid_ref, plus_ref, minus_ref, stats_ref, *scratch = outs
    pair = mid_ref.shape[0]
    marks = mid_ref.shape[1]
    dh = pair // 2
    segments = early_ref.shape[0] // WIN
    z = place_ref[0]
    last = place_ref[1] - 1
    if ring:
        stack_ref = scratch[0]
        collect(land_refs[0], land_refs[1:], stack_ref, z, marks)
        halos = {0: land_refs[1][:pair, marks:], segments - 1: land_refs[-1][:pair, marks:]}
    else:
        stack_ref = land_refs[0]
        halos = {0: land_refs[1][...], segments - 1: land_refs[2][...]}
    groups = stack_ref.shape[0]

    peaks, totals = [], []
    for j in range(groups):
        tail = stack_ref[j, pair:, :].astype(F32)
        peaks.append(tail[0:1] + tail[1:2] + tail[2:3])
        totals.append(tail[3:4] + tail[4:5])
    peak = functools.reduce(jnp.maximum, peaks)
    total = jnp.zeros_like(peak)
    sums = jnp.zeros((pair, marks), F32)
    for j in range(groups):
        factor = jnp.exp(peaks[j] - peak)
        total = total + factor * totals[j]
        sums = sums + factor * stack_ref[j, :pair, :].astype(F32)
    inv_total = 1.0 / total
    mean = sums * inv_total
    normed, inverse = [], []
    for half in range(2):
        block = mean[half * dh : (half + 1) * dh]
        centred = block - jnp.mean(block, axis=0, keepdims=True)
        variance = jnp.mean(centred * centred, axis=0, keepdims=True)
        inv = 1.0 / jnp.sqrt(variance + EPS)
        normed.append(centred * inv)
        inverse.append(inv)
    normed = jnp.concatenate(normed, axis=0)
    land_f = normed * spread(affine_ref[:pair], marks) + spread(affine_ref[pair:], marks)
    land_t = land_f.astype(BF)
    land = land_f.T.astype(BF)
    own_tail = stack_ref[z, pair:, :].astype(F32)
    own_peak = own_tail[0:1] + own_tail[1:2] + own_tail[2:3]
    factor = jnp.exp(own_peak - peak) * inv_total
    stats_ref[:pair] = normed
    stats_ref[pair : 2 * pair] = mean
    r8 = rows((8, marks))
    stats_ref[2 * pair :] = jnp.where(r8 == 0, inverse[0], jnp.where(r8 == 1, inverse[1], factor))

    land_grad = jnp.zeros((pair, marks), F32)
    halo_grads = {}
    low = lanes((WIN, pair)) < dh
    for s in range(segments):
        span = slice(s * WIN, (s + 1) * WIN)
        a = a_ref[2 * s * WIN : 2 * (s + 1) * WIN]
        early, top_e, sum_e, part_e = (
            early_ref[span, slot * pair : (slot + 1) * pair] for slot in range(4)
        )
        sl = dot(a, land_t)
        scores, grads = sl[:WIN], sl[WIN:]
        top = jnp.maximum(row_max(scores), top_e)
        if s in halos:
            sh = dot(a, halos[s], NT)
            outside = z == (0 if s == 0 else last)
            scores_h, grads_h = jnp.where(outside, NEG, sh[:WIN]), sh[WIN:]
            top = jnp.maximum(top, row_max(scores_h))
        expo = jnp.exp(scores - spread(top, marks))
        scale_e = jnp.exp(top_e - top)
        total_row = row_sum(expo) + sum_e * scale_e
        part = part_e * scale_e
        out = early * scale_e
        if s in halos:
            expo_h = jnp.exp(scores_h - top)
            total_row = total_row + row_sum(expo_h)
            part = part + row_sum(expo_h.astype(BF).astype(F32) * grads_h)
        inv = 1.0 / total_row
        probs = expo * spread(inv, marks)
        probs_b = probs.astype(BF)
        delta = row_sum(probs_b.astype(F32) * grads) + part * inv
        b = jnp.concatenate([(probs * (grads - spread(delta, marks))).astype(BF), probs_b], axis=0)
        od = dot(b, land)
        at = at_ref[s * pair : (s + 1) * pair]
        if s in halos:
            probs_h = expo_h * inv
            b_h = jnp.concatenate(
                [(probs_h * (grads_h - delta)).astype(BF), probs_h.astype(BF)], axis=0
            )
            od = od + dot(b_h, halos[s])
            halo_grads[s] = dot(at, b_h).astype(BF)
        late_ref[span] = jnp.where(low, od[:WIN], od[WIN:] + out * inv)
        rows_ref[span, :pair] = top + jnp.log(total_row)
        rows_ref[span, pair:] = delta
        land_grad = land_grad + dot(at, b)
    land_b = land_grad.astype(BF)
    mid_ref[...] = land_b
    if ring:
        plus_ref[:, :marks] = land_b
        minus_ref[:, :marks] = land_b
        plus_ref[:, marks:] = halo_grads[segments - 1]
        minus_ref[:, marks:] = halo_grads[0]
    else:
        plus_ref[...] = halo_grads[segments - 1]
        minus_ref[...] = halo_grads[0]


def window_backward_kernel(x_ref, a_ref, at_ref, late_ref, rows_ref, od_ref, dkvt_ref, *, scale):
    count, width = x_ref.shape
    pair = width // 2
    dh = pair // 2
    segments = count // WIN
    dkvt_ref[...] = jnp.zeros(dkvt_ref.shape, F32)
    low = lanes((WIN, pair)) < dh
    for s in range(segments):
        span = slice(s * WIN, (s + 1) * WIN)
        near = slice(max(s - 1, 0) * WIN, min(s + 2, segments) * WIN)
        a = a_ref[2 * s * WIN : 2 * (s + 1) * WIN]
        kvw = x_ref[near, :pair]
        reach = near.stop - near.start
        sw = dot(a, kvw, NT)
        probs = jnp.exp(sw[:WIN] - spread(rows_ref[span, :pair], reach))
        grad_b = (probs * (sw[WIN:] - spread(rows_ref[span, pair:], reach))).astype(BF)
        late = late_ref[span]
        dq = (dot(grad_b, kvw) + late) * scale
        od_ref[span] = jnp.where(low, dq, late).astype(BF)
        b = jnp.concatenate([grad_b, probs.astype(BF)], axis=0)
        dkvt_ref[:, near] += dot(at_ref[s * pair : (s + 1) * pair], b)


def final_kernel(*refs, ring, sub, parts, tiled):
    grads_in = ring + 1 if ring else 1
    place_ref = refs[0]
    grad_refs = refs[1 : 1 + grads_in]
    rest = refs[1 + grads_in :]
    if ring:
        prev_src, next_src = grad_refs[1], grad_refs[-1]
    else:
        prev_src, next_src, *rest = rest
    x_ref, w_ref, affine_ref, expo_ref, od_ref, dkvt_ref, stats_ref, *outs = rest
    send_ref = outs[0]
    count, width = x_ref.shape
    pair = width // 2
    dh = pair // 2
    marks = expo_ref.shape[1]
    if ring:
        stack_ref = outs[-1]
        collect(grad_refs[0], grad_refs[1:], stack_ref, place_ref[0], marks)
    else:
        stack_ref = grad_refs[0]
    z = place_ref[0]
    from_prev = prev_src[:, prev_src.shape[1] - pair :].astype(F32)
    from_next = next_src[:, next_src.shape[1] - pair :].astype(F32)
    from_prev = jnp.where(z == 0, 0.0, from_prev)
    from_next = jnp.where(z == place_ref[1] - 1, 0.0, from_next)
    grad = stack_ref[0].astype(F32)
    for j in range(1, stack_ref.shape[0]):
        grad = grad + stack_ref[j].astype(F32)
    normed = stats_ref[:pair]
    mean = stats_ref[pair : 2 * pair]
    factor = stats_ref[2 * pair + 2 : 2 * pair + 3]
    gained = grad * spread(affine_ref[:pair], marks)
    blocks = []
    for half in range(2):
        part = slice(half * dh, (half + 1) * dh)
        g = gained[part]
        first = jnp.mean(g, axis=0, keepdims=True)
        second = jnp.mean(g * normed[part], axis=0, keepdims=True)
        inv = stats_ref[2 * pair + half : 2 * pair + half + 1]
        blocks.append(inv * (g - first - normed[part] * second))
    grad_mean = jnp.concatenate(blocks, axis=0)
    grad_b = grad_mean.astype(BF)
    column = jnp.sum(grad_b.astype(F32) * mean, axis=0, keepdims=True)
    scaled = (grad_mean * factor).astype(BF)

    gain_sum = jnp.sum(grad * normed, axis=1, keepdims=True)
    bias_sum = jnp.sum(grad, axis=1, keepdims=True)
    lane = lanes((pair, pair))
    square = jnp.where(lane == 0, gain_sum, jnp.where(lane == 1, bias_sum, 0.0)).T
    norm_hi = square[:8].astype(BF)
    norm_lo = (square[:8] - norm_hi.astype(F32)).astype(BF)
    norm_rows = jnp.concatenate(
        [
            jnp.concatenate([norm_hi, norm_lo], axis=1),
        ],
        axis=0,
    )

    kv = x_ref[:, :pair]
    wide = widen_proj(w_ref[place_ref[2]])
    expo_b = expo_ref[...]
    weights = expo_b.astype(F32) * factor
    grad_logit = (weights * (dot(kv, grad_b) - column)).astype(BF)
    land = dot(expo_b, scaled, NT) + dot(grad_logit, wide, NT)
    window = dkvt_ref[...].T
    dests, out_rows, _ = send_ref.shape
    step = count // dests
    dkv = land + window
    head_fix = from_prev.T
    tail_fix = from_next.T
    for d in range(dests):
        span = slice(d * step, (d + 1) * step)
        block = dkv[span]
        fix_top = head_fix if d == 0 else None
        fix_end = tail_fix if d == dests - 1 else None
        for at in range(0, step, WIN):
            piece = block[at : at + WIN]
            if fix_top is not None and at == 0:
                piece = piece + fix_top
            if fix_end is not None and at + WIN == step:
                piece = piece + fix_end
            send_ref[d, at : at + WIN, :pair] = piece.astype(BF)
        send_ref[d, :step, pair:] = od_ref[span]
        send_ref[d, out_rows - 8 :] = norm_rows
    kvt = kv.T
    group = count // sub
    for sb in range(sub):
        span = slice(sb * group, (sb + 1) * group)
        proj = dot(kvt[:, span], grad_logit[span])[:dh]
        if tiled:
            wide_part = marks // parts
            quarter = dh // 4
            for i in range(parts):
                tile = proj[:, i * wide_part : (i + 1) * wide_part].astype(BF)
                for k in range(4):
                    send_ref[
                        sb * parts + i, step : out_rows - 8, k * dh : (k + 1) * dh
                    ] = tile[k * quarter : (k + 1) * quarter]
        else:
            outs[1][...] = proj


def unpack_kernel(r_ref, att_ref, dq_ref, dk_ref, dv_ref, norm_ref, *proj_refs):
    heads, _, width = r_ref.shape
    dh = width // 4
    pair = 2 * dh
    step = att_ref.shape[0]
    for h in range(heads):
        cols = slice(h * dh, (h + 1) * dh)
        for slot, ref in enumerate((dk_ref, dv_ref, dq_ref, att_ref)):
            ref[:, cols] = r_ref[h, :step, slot * dh : (slot + 1) * dh]
    norm = jnp.zeros((8, pair), F32)
    for h in range(heads):
        block = r_ref[h, r_ref.shape[1] - 8 :, :].astype(F32)
        norm = norm + (block[:, :pair] + block[:, pair:])
    norm_ref[0:1] = norm[0:1, :dh]
    norm_ref[1:2] = norm[1:2, :dh]
    norm_ref[2:3] = norm[0:1, dh:]
    norm_ref[3:4] = norm[1:2, dh:]
    if proj_refs:
        proj_ref = proj_refs[0]
        quarter = dh // 4
        for h in range(heads):
            for k in range(4):
                proj_ref[0, h, k * quarter : (k + 1) * quarter] = r_ref[
                    h, step : r_ref.shape[1] - 8, k * dh : (k + 1) * dh
                ].astype(F32)


def shape_of(shape, dtype):
    return jax.ShapeDtypeStruct(shape, dtype)


VM = pl.BlockSpec(memory_space=pltpu.VMEM)
SM = pl.BlockSpec(memory_space=pltpu.SMEM)
ANY = pl.BlockSpec(memory_space=pltpu.HBM)


def call(kernel, out_shape, args, specs, name, scratch=(), keep=True, flops=0):
    args = [
        arg if spec is SM else pltpu.with_memory_space_constraint(arg, spec.memory_space)
        for arg, spec in zip(args, specs)
    ]
    if keep:
        out_shape = jax.tree.map(lambda s: pltpu.VMEM(s.shape, s.dtype), out_shape)
    cost = pl.CostEstimate(flops=flops, bytes_accessed=0, transcendentals=0) if flops else None
    return pl.pallas_call(
        kernel,
        out_shape=out_shape,
        in_specs=specs,
        out_specs=jax.tree.map(lambda _: VM, out_shape),
        scratch_shapes=scratch,
        compiler_params=pltpu.CompilerParams(vmem_limit_bytes=VMEM_LIMIT),
        cost_estimate=cost,
        name=name,
    )(*args)


def per_device(queries, keys, values, w_proj, ln_gain, ln_bias, cotangent):
    tokens_dev, features = queries.shape
    heads, dh, marks = w_proj.shape
    pair = 2 * dh
    width = 4 * dh
    count = tokens_dev * heads
    scale = 1.0 / math.sqrt(dh)
    seqs = lax.axis_size(SEQ)
    sub = lax.axis_size("sub")
    parts = lax.axis_size("part")
    halves = lax.axis_size("half")
    head = lax.axis_index(HEAD).astype(jnp.int32)
    z = lax.axis_index(SEQ).astype(jnp.int32)
    place = jnp.stack([z, jnp.int32(seqs), head])
    ring = seqs - 1 if 3 <= seqs <= 8 else 0
    wide_part = marks // parts
    tiled = halves == 1 and wide_part == dh and dh % 64 == 0

    packed = call(
        pack_kernel,
        shape_of((heads, tokens_dev, width), BF),
        (queries, keys, values, cotangent),
        [ANY] * 4,
        "pack",
        [pltpu.VMEM((4, tokens_dev, features), BF), pltpu.SemaphoreType.DMA((4,))],
    )
    x = lax.all_to_all(packed, HEAD, 0, 0, tiled=True).reshape(count, width)

    rows_out = pair + EXTRA
    out_shape = [shape_of((rows_out, marks), BF)]
    if ring:
        out_shape += [shape_of((rows_out, marks + pair), BF)] * 2
    out_shape.append(shape_of((count, marks), BF))
    mid, *halo_outs, expo = call(
        local_sums_kernel, out_shape, (place, x, w_proj), [SM, VM, VM], "local_sums"
    )

    def shifted(block, shift):
        return lax.ppermute(block, SEQ, [(i, (i + shift) % seqs) for i in range(seqs)])

    def forward(block, shift):
        route = [(i, i + shift) for i in range(seqs) if 0 <= i + shift < seqs]
        return lax.ppermute(block, SEQ, route)

    if ring:
        recv = [shifted(halo_outs[0], 1)]
        recv += [shifted(mid, k) for k in range(2, ring)]
        recv += [shifted(halo_outs[1], ring)]
        lands = [mid, *recv]
        halos = [recv[0], recv[-1]]
    else:
        halos = [forward(x[count - WIN :, :pair], 1), forward(x[:WIN, :pair], -1)]
        lands = [lax.all_gather(mid, SEQ), *halos]
    halo_wide = marks + pair if ring else pair
    work = 2 * count * 3 * WIN * pair
    early, a_all, at_all, affine = call(
        functools.partial(window_forward_kernel, scale=scale),
        [
            shape_of((count, 4 * pair), F32),
            shape_of((2 * count, pair), BF),
            shape_of((count // WIN * pair, 2 * WIN), BF),
            shape_of((2 * pair, pair), F32),
        ],
        (x, ln_gain, ln_bias),
        [VM] * 3,
        "window_forward",
        flops=3 * work,
    )
    late, row_stats, grad_mid, plus, minus, stats = call(
        functools.partial(landmark_forward_kernel, ring=ring),
        [
            shape_of((count, pair), F32),
            shape_of((count, 2 * pair), F32),
            shape_of((pair, marks), BF),
            shape_of((pair, halo_wide), BF),
            shape_of((pair, halo_wide), BF),
            shape_of((2 * pair + 8, marks), F32),
        ],
        (place, early, a_all, at_all, *lands, affine),
        [SM] + [VM] * (len(lands) + 4),
        "landmark_forward",
        [pltpu.VMEM((seqs, rows_out, marks), BF)] if ring else [],
    )
    if ring:
        grads = [grad_mid, shifted(plus, 1)]
        grads += [shifted(grad_mid, k) for k in range(2, ring)]
        grads += [shifted(minus, ring)]
    else:
        grads = [lax.all_gather(grad_mid, SEQ), forward(plus, 1), forward(minus, -1)]
    od, dkvt = call(
        functools.partial(window_backward_kernel, scale=scale),
        [shape_of((count, pair), BF), shape_of((pair, count), F32)],
        (x, a_all, at_all, late, row_stats),
        [VM] * 5,
        "window_backward",
        flops=5 * work,
    )
    send_rows = tokens_dev + 8 + (dh // 4 if tiled else 0)
    out_shape = [shape_of((heads, send_rows, width), BF)]
    if not tiled:
        out_shape.append(shape_of((dh, marks), F32))
    send, *proj = call(
        functools.partial(
            final_kernel, ring=ring, sub=sub if tiled else 1, parts=parts, tiled=tiled
        ),
        out_shape,
        (place, *grads, x, w_proj, affine, expo, od, dkvt, stats),
        [SM] + [VM] * (len(grads) + 7),
        "landmark_backward",
        [pltpu.VMEM((seqs, pair, marks), BF)] if ring else [],
    )
    back = lax.all_to_all(send, HEAD, 0, 0, tiled=True)
    out_shape = [shape_of((tokens_dev, features), BF)] * 4 + [shape_of((4, dh), F32)]
    if tiled:
        out_shape.append(shape_of((1, heads, dh, wide_part), F32))
    attended, dq, dk, dv, grad_norm, *tiles = call(
        unpack_kernel, out_shape, (back,), [VM], "unpack", keep=False
    )
    if tiled:
        grad_proj = tiles[0]
    else:
        full = lax.all_gather(proj[0], HEAD)
        inner = ("half", "part") if halves > 1 else "part"
        grad_proj = lax.psum_scatter(full, inner, scatter_dimension=2, tiled=True)[None] / parts
    return (attended, dq, dk, dv, grad_proj, grad_norm)


def solution(mesh):
    ctx, inner = mesh.shape["ctx"], mesh.shape["inner"]

    def whole(queries, keys, values, w_proj, ln_gain, ln_bias, cotangent):
        heads = w_proj.shape[0]
        part = min(heads, inner)
        sub = heads // part
        order = np.asarray(mesh.devices).reshape(ctx // sub, sub, inner // part, part)
        split = Mesh(order, ("seq", "sub", "half", "part"))
        every = P(("seq", "sub", "half", "part"), None)
        return jax.shard_map(
            per_device,
            mesh=split,
            in_specs=(every, every, every, P(), P(), P(), every),
            out_specs=(
                every,
                every,
                every,
                every,
                P(("seq", "sub"), None, None, ("half", "part")),
                P(),
            ),
            check_vma=False,
        )(queries, keys, values, w_proj, ln_gain, ln_bias, cotangent)

    return whole
```

```python
import functools
import math

import jax
import jax.numpy as jnp
import numpy as np
from jax import lax
from jax.experimental import pallas as pl
from jax.experimental.pallas import tpu as pltpu
from jax.sharding import Mesh
from jax.sharding import PartitionSpec as P

WIN = 128
EXTRA = 8
EPS = 1e-05
NEG = -1e30
BATCH = 8
VMEM_LIMIT = 24 * 1024 * 1024
BF = jnp.bfloat16
F32 = jnp.float32

NN = (((1,), (0,)), ((), ()))
NT = (((1,), (1,)), ((), ()))
SEQ = ("seq", "half")
HEAD = ("sub", "part")


def dot(a, b, dims=NN):
    return lax.dot_general(a, b, dims, preferred_element_type=F32)


def lanes(shape):
    return lax.broadcasted_iota(jnp.int32, shape, 1)


def rows(shape):
    return lax.broadcasted_iota(jnp.int32, shape, 0)


def pack_kernel(z_ref, head_ref, q_ref, k_ref, v_ref, g_ref, o_ref, buffer_ref, sems):
    heads, _, width = o_ref.shape
    dh = width // 4
    del z_ref, head_ref
    copies = []
    for slot, ref in enumerate((k_ref, v_ref, q_ref, g_ref)):
        copy = pltpu.make_async_copy(ref, buffer_ref.at[slot], sems.at[slot])
        copy.start()
        copies.append(copy)
    for slot, copy in enumerate(copies):
        copy.wait()
        for h in range(heads):
            o_ref[h, :, slot * dh : (slot + 1) * dh] = buffer_ref[slot, :, h * dh : (h + 1) * dh]


def split_rows(total_rows, width, pieces):
    r = rows((total_rows, width))
    out = jnp.zeros((total_rows, width), F32)
    for index, piece in enumerate(pieces):
        out = jnp.where(r == index, piece, out)
    return out.astype(BF)


def bf_pieces(x, count):
    out = []
    for _ in range(count):
        piece = x.astype(BF).astype(F32)
        out.append(piece)
        x = x - piece
    return out


def widen_proj(w):
    return jnp.concatenate([w, jnp.zeros_like(w)], axis=0)


def local_sums_kernel(head_ref, x_ref, w_ref, mid_ref, *out_refs):
    expo_ref = out_refs[-1]
    pair = x_ref.shape[1] // 2
    kv = x_ref[:, :pair]
    logits = dot(kv, widen_proj(w_ref[head_ref[0]]))
    peak = jnp.max(logits, axis=0, keepdims=True)
    expo = jnp.exp(logits - peak)
    total = jnp.sum(expo, axis=0, keepdims=True)
    expo_b = expo.astype(BF)
    expo_ref[...] = expo_b
    sums = dot(kv.T, expo_b).astype(BF)
    marks = sums.shape[1]
    tail = split_rows(EXTRA, marks, bf_pieces(peak, 3) + bf_pieces(total, 2))
    targets = [(mid_ref, None)]
    if len(out_refs) == 3:
        count = x_ref.shape[0]
        targets += [(out_refs[0], kv[count - WIN :]), (out_refs[1], kv[:WIN])]
    for ref, halo in targets:
        ref[:pair, :marks] = sums
        ref[pair:, :marks] = tail
        if halo is not None:
            ref[:pair, marks:] = halo
            ref[pair:, marks:] = jnp.zeros((EXTRA, pair), BF)


def collect(own_ref, recv_refs, stack_ref, index, marks):
    count = len(recv_refs) + 1
    stack_ref[index] = own_ref[...]
    for shift, ref in enumerate(recv_refs, start=1):
        stack_ref[lax.rem(index + (count - shift), count)] = ref[:, :marks]


def as_column(ref):
    row = jnp.concatenate([ref[0:1, :], ref[1:2, :]], axis=1)
    size = row.shape[1]
    return jnp.sum(
        jnp.where(rows((size, size)) == lanes((size, size)), row, 0.0), axis=1, keepdims=True
    )


def spread(x, width):
    return jnp.concatenate([x] * (width // x.shape[1]), axis=1)


def row_max(x):
    return jnp.max(x, axis=1, keepdims=True)


def row_sum(x):
    return jnp.sum(x, axis=1, keepdims=True)


def window_forward_kernel(x_ref, gain_src, bias_src, early_ref, a_ref, at_ref, affine_ref, *, scale):
    count, width = x_ref.shape
    pair = width // 2
    dh = pair // 2
    segments = count // WIN
    low = lanes((WIN, pair)) < dh
    zero_b = jnp.zeros((WIN, pair), BF)
    for slot, src in enumerate((gain_src, bias_src)):
        affine_ref[slot * pair : (slot + 1) * pair] = jnp.broadcast_to(
            as_column(src), (pair, affine_ref.shape[1])
        )
    for s in range(segments):
        qg = x_ref[s * WIN : (s + 1) * WIN, pair:]
        q0 = jnp.where(low, (qg.astype(F32) * scale).astype(BF), zero_b)
        g0 = jnp.where(low, zero_b, qg)
        a = jnp.concatenate([q0, g0], axis=0)
        a_ref[2 * s * WIN : 2 * (s + 1) * WIN] = a
        at_ref[:, 2 * s * WIN : 2 * (s + 1) * WIN] = a.T
        kvw = x_ref[max(s - 1, 0) * WIN : min(s + 2, segments) * WIN, :pair]
        sw = dot(a, kvw, NT)
        scores, grads = sw[:WIN], sw[WIN:]
        top = row_max(scores)
        expo = jnp.exp(scores - top)
        expo_b = expo.astype(BF)
        out = dot(expo_b, kvw)
        part = row_sum(expo * grads)
        span = slice(s * WIN, (s + 1) * WIN)
        early_ref[span, :pair] = out
        for slot, stat in enumerate((top, row_sum(expo), part), start=1):
            early_ref[span, slot * pair : (slot + 1) * pair] = jnp.broadcast_to(stat, out.shape)


def landmark_forward_kernel(*refs, ring, seqs):
    lands = ring + 1 if ring else 3
    z_ref, early_ref, a_ref, at_ref = refs[:4]
    land_refs = refs[4 : 4 + lands]
    affine_ref = refs[4 + lands]
    outs = refs[5 + lands :]
    late_ref, rows_ref, mid_ref, plus_ref, minus_ref, stats_ref, *scratch = outs
    pair = mid_ref.shape[0]
    marks = mid_ref.shape[1]
    dh = pair // 2
    segments = early_ref.shape[0] // WIN
    z = z_ref[0]
    last = seqs - 1
    if ring:
        stack_ref = scratch[0]
        collect(land_refs[0], land_refs[1:], stack_ref, z, marks)
        halos = {0: land_refs[1][:pair, marks:], segments - 1: land_refs[-1][:pair, marks:]}
    else:
        stack_ref = land_refs[0]
        halos = {0: land_refs[1][...], segments - 1: land_refs[2][...]}
    groups = stack_ref.shape[0]

    peaks, totals = [], []
    for j in range(groups):
        tail = stack_ref[j, pair:, :].astype(F32)
        peaks.append(tail[0:1] + tail[1:2] + tail[2:3])
        totals.append(tail[3:4] + tail[4:5])
    peak = functools.reduce(jnp.maximum, peaks)
    total = jnp.zeros_like(peak)
    factors = [jnp.exp(p - peak) for p in peaks]
    for factor, part in zip(factors, totals):
        total = total + factor * part
    inv_total = 1.0 / total
    factors = [factor * inv_total for factor in factors]
    land_t, inverse = [], []
    for half in range(2):
        block = slice(half * dh, (half + 1) * dh)
        mean = factors[0] * stack_ref[0, block, :].astype(F32)
        for j in range(1, groups):
            mean = mean + factors[j] * stack_ref[j, block, :].astype(F32)
        stats_ref[pair + half * dh : pair + (half + 1) * dh] = mean
        centred = mean - jnp.mean(mean, axis=0, keepdims=True)
        inv = 1.0 / jnp.sqrt(jnp.mean(centred * centred, axis=0, keepdims=True) + EPS)
        normed = centred * inv
        stats_ref[block] = normed
        inverse.append(inv)
        gain = affine_ref[half * dh : (half + 1) * dh]
        bias = affine_ref[pair + half * dh : pair + (half + 1) * dh]
        land_t.append((normed * spread(gain, marks) + spread(bias, marks)).astype(BF))
    land_t = jnp.concatenate(land_t, axis=0)
    land = land_t.T
    own_tail = stack_ref[z, pair:, :].astype(F32)
    own_peak = own_tail[0:1] + own_tail[1:2] + own_tail[2:3]
    factor = jnp.exp(own_peak - peak) * inv_total
    r8 = rows((8, marks))
    stats_ref[2 * pair :] = jnp.where(r8 == 0, inverse[0], jnp.where(r8 == 1, inverse[1], factor))

    low = lanes((WIN, pair)) < dh
    land_grad = jnp.zeros((pair, marks), F32)
    halo_grads = {}
    for first in range(0, segments, BATCH):
        batch = range(first, min(first + BATCH, segments))
        spans = {s: slice(s * WIN, (s + 1) * WIN) for s in batch}
        blocks = {s: a_ref[2 * s * WIN : 2 * (s + 1) * WIN] for s in batch}
        early = {
            s: [early_ref[spans[s], slot * pair : (slot + 1) * pair] for slot in range(4)]
            for s in batch
        }
        sl = {s: dot(blocks[s], land_t) for s in batch}
        sh = {s: dot(blocks[s], halos[s], NT) for s in batch if s in halos}
        scores = {s: sl[s][:WIN] for s in batch}
        grads = {s: sl[s][WIN:] for s in batch}
        scores_h = {
            s: jnp.where(z == (0 if s == 0 else last), NEG, sh[s][:WIN]) for s in sh
        }
        top = {s: jnp.maximum(row_max(scores[s]), early[s][1]) for s in batch}
        for s in sh:
            top[s] = jnp.maximum(top[s], row_max(scores_h[s]))
        expo = {s: jnp.exp(scores[s] - spread(top[s], marks)) for s in batch}
        expo_h = {s: jnp.exp(scores_h[s] - top[s]) for s in sh}
        scale_e = {s: jnp.exp(early[s][1] - top[s]) for s in batch}
        total_row, part = {}, {}
        for s in batch:
            total_row[s] = row_sum(expo[s]) + early[s][2] * scale_e[s]
            part[s] = row_sum(expo[s] * grads[s]) + early[s][3] * scale_e[s]
            if s in sh:
                total_row[s] = total_row[s] + row_sum(expo_h[s])
                part[s] = part[s] + row_sum(expo_h[s] * sh[s][WIN:])
        inv = {s: 1.0 / total_row[s] for s in batch}
        delta = {s: part[s] * inv[s] for s in batch}
        b, b_h = {}, {}
        for s in batch:
            probs = expo[s] * spread(inv[s], marks)
            b[s] = jnp.concatenate(
                [(probs * (grads[s] - spread(delta[s], marks))).astype(BF), probs.astype(BF)],
                axis=0,
            )
            rows_ref[spans[s], :pair] = top[s] + jnp.log(total_row[s])
            rows_ref[spans[s], pair:] = delta[s]
        for s in sh:
            probs = expo_h[s] * inv[s]
            b_h[s] = jnp.concatenate(
                [(probs * (sh[s][WIN:] - delta[s])).astype(BF), probs.astype(BF)], axis=0
            )
        for s in batch:
            od = dot(b[s], land)
            if s in sh:
                od = od + dot(b_h[s], halos[s])
            late_ref[spans[s]] = jnp.where(
                low, od[:WIN], od[WIN:] + early[s][0] * (scale_e[s] * inv[s])
            )
        reach = slice(2 * batch[0] * WIN, 2 * (batch[-1] + 1) * WIN)
        land_grad = land_grad + dot(at_ref[:, reach], jnp.concatenate([b[s] for s in batch], axis=0))
        for s in sh:
            halo_grads[s] = dot(at_ref[:, 2 * s * WIN : 2 * (s + 1) * WIN], b_h[s]).astype(BF)
    land_b = land_grad.astype(BF)
    mid_ref[...] = land_b
    if ring:
        plus_ref[:, :marks] = land_b
        minus_ref[:, :marks] = land_b
        plus_ref[:, marks:] = halo_grads[segments - 1]
        minus_ref[:, marks:] = halo_grads[0]
    else:
        plus_ref[...] = halo_grads[segments - 1]
        minus_ref[...] = halo_grads[0]


def window_backward_kernel(x_ref, a_ref, at_ref, late_ref, rows_ref, od_ref, dkvt_ref, *, scale):
    count, width = x_ref.shape
    pair = width // 2
    dh = pair // 2
    segments = count // WIN
    dkvt_ref[...] = jnp.zeros(dkvt_ref.shape, F32)
    low = lanes((WIN, pair)) < dh
    for s in range(segments):
        span = slice(s * WIN, (s + 1) * WIN)
        near = slice(max(s - 1, 0) * WIN, min(s + 2, segments) * WIN)
        a = a_ref[2 * s * WIN : 2 * (s + 1) * WIN]
        kvw = x_ref[near, :pair]
        reach = near.stop - near.start
        sw = dot(a, kvw, NT)
        probs = jnp.exp(sw[:WIN] - spread(rows_ref[span, :pair], reach))
        grad_b = (probs * (sw[WIN:] - spread(rows_ref[span, pair:], reach))).astype(BF)
        late = late_ref[span]
        dq = (dot(grad_b, kvw) + late) * scale
        od_ref[span] = jnp.where(low, dq, late).astype(BF)
        b = jnp.concatenate([grad_b, probs.astype(BF)], axis=0)
        dkvt_ref[:, near] += dot(at_ref[:, 2 * s * WIN : 2 * (s + 1) * WIN], b)


def final_kernel(*refs, ring, seqs, sub, parts, tiled):
    grads_in = ring + 1 if ring else 1
    z_ref, head_ref = refs[:2]
    grad_refs = refs[2 : 2 + grads_in]
    rest = refs[2 + grads_in :]
    if ring:
        prev_src, next_src = grad_refs[1], grad_refs[-1]
    else:
        prev_src, next_src, *rest = rest
    x_ref, w_ref, affine_ref, expo_ref, od_ref, dkvt_ref, stats_ref, *outs = rest
    send_ref = outs[0]
    count, width = x_ref.shape
    pair = width // 2
    dh = pair // 2
    marks = expo_ref.shape[1]
    if ring:
        stack_ref = outs[-1]
        collect(grad_refs[0], grad_refs[1:], stack_ref, z_ref[0], marks)
    else:
        stack_ref = grad_refs[0]
    z = z_ref[0]
    from_prev = prev_src[:, prev_src.shape[1] - pair :].astype(F32)
    from_next = next_src[:, next_src.shape[1] - pair :].astype(F32)
    from_prev = jnp.where(z == 0, 0.0, from_prev)
    from_next = jnp.where(z == seqs - 1, 0.0, from_next)
    grad = stack_ref[0].astype(F32)
    for j in range(1, stack_ref.shape[0]):
        grad = grad + stack_ref[j].astype(F32)
    normed = stats_ref[:pair]
    mean = stats_ref[pair : 2 * pair]
    factor = stats_ref[2 * pair + 2 : 2 * pair + 3]
    gained = grad * spread(affine_ref[:pair], marks)
    blocks = []
    for half in range(2):
        part = slice(half * dh, (half + 1) * dh)
        g = gained[part]
        first = jnp.mean(g, axis=0, keepdims=True)
        second = jnp.mean(g * normed[part], axis=0, keepdims=True)
        inv = stats_ref[2 * pair + half : 2 * pair + half + 1]
        blocks.append(inv * (g - first - normed[part] * second))
    grad_mean = jnp.concatenate(blocks, axis=0)
    grad_b = grad_mean.astype(BF)
    column = jnp.sum(grad_b.astype(F32) * mean, axis=0, keepdims=True)
    scaled = (grad_mean * factor).astype(BF)

    gain_sum = jnp.sum(grad * normed, axis=1, keepdims=True)
    bias_sum = jnp.sum(grad, axis=1, keepdims=True)
    lane = lanes((pair, pair))
    square = jnp.where(lane == 0, gain_sum, jnp.where(lane == 1, bias_sum, 0.0)).T
    norm_hi = square[:8].astype(BF)
    norm_lo = (square[:8] - norm_hi.astype(F32)).astype(BF)
    norm_rows = jnp.concatenate(
        [
            jnp.concatenate([norm_hi, norm_lo], axis=1),
        ],
        axis=0,
    )

    kv = x_ref[:, :pair]
    wide = widen_proj(w_ref[head_ref[0]])
    expo_b = expo_ref[...]
    weights = expo_b.astype(F32) * factor
    grad_logit = (weights * (dot(kv, grad_b) - column)).astype(BF)
    land = dot(expo_b, scaled, NT) + dot(grad_logit, wide, NT)
    window = dkvt_ref[...].T
    dests, out_rows, _ = send_ref.shape
    step = count // dests
    dkv = land + window
    head_fix = from_prev.T
    tail_fix = from_next.T
    for d in range(dests):
        span = slice(d * step, (d + 1) * step)
        block = dkv[span]
        fix_top = head_fix if d == 0 else None
        fix_end = tail_fix if d == dests - 1 else None
        for at in range(0, step, WIN):
            piece = block[at : at + WIN]
            if fix_top is not None and at == 0:
                piece = piece + fix_top
            if fix_end is not None and at + WIN == step:
                piece = piece + fix_end
            send_ref[d, at : at + WIN, :pair] = piece.astype(BF)
        send_ref[d, :step, pair:] = od_ref[span]
        send_ref[d, out_rows - 8 :] = norm_rows
    kvt = kv.T
    group = count // sub
    for sb in range(sub):
        span = slice(sb * group, (sb + 1) * group)
        proj = dot(kvt[:, span], grad_logit[span])[:dh]
        if tiled:
            wide_part = marks // parts
            quarter = dh // 4
            for i in range(parts):
                tile = proj[:, i * wide_part : (i + 1) * wide_part].astype(BF)
                for k in range(4):
                    send_ref[
                        sb * parts + i, step : out_rows - 8, k * dh : (k + 1) * dh
                    ] = tile[k * quarter : (k + 1) * quarter]
        else:
            outs[1][...] = proj


def unpack_kernel(r_ref, att_ref, dq_ref, dk_ref, dv_ref, norm_ref, *proj_refs):
    heads, _, width = r_ref.shape
    dh = width // 4
    pair = 2 * dh
    step = att_ref.shape[0]
    for h in range(heads):
        cols = slice(h * dh, (h + 1) * dh)
        for slot, ref in enumerate((dk_ref, dv_ref, dq_ref, att_ref)):
            ref[:, cols] = r_ref[h, :step, slot * dh : (slot + 1) * dh]
    norm = jnp.zeros((8, pair), F32)
    for h in range(heads):
        block = r_ref[h, r_ref.shape[1] - 8 :, :].astype(F32)
        norm = norm + (block[:, :pair] + block[:, pair:])
    norm_ref[0:1] = norm[0:1, :dh]
    norm_ref[1:2] = norm[1:2, :dh]
    norm_ref[2:3] = norm[0:1, dh:]
    norm_ref[3:4] = norm[1:2, dh:]
    if proj_refs:
        proj_ref = proj_refs[0]
        quarter = dh // 4
        for h in range(heads):
            for k in range(4):
                proj_ref[0, h, k * quarter : (k + 1) * quarter] = r_ref[
                    h, step : r_ref.shape[1] - 8, k * dh : (k + 1) * dh
                ].astype(F32)


def shape_of(shape, dtype):
    return jax.ShapeDtypeStruct(shape, dtype)


VM = pl.BlockSpec(memory_space=pltpu.VMEM)
SM = pl.BlockSpec(memory_space=pltpu.SMEM)
ANY = pl.BlockSpec(memory_space=pltpu.HBM)


def call(kernel, out_shape, args, specs, name, scratch=(), keep=True, flops=0):
    args = [
        arg if spec is SM else pltpu.with_memory_space_constraint(arg, spec.memory_space)
        for arg, spec in zip(args, specs)
    ]
    if keep:
        out_shape = jax.tree.map(lambda s: pltpu.VMEM(s.shape, s.dtype), out_shape)
    cost = pl.CostEstimate(flops=flops, bytes_accessed=0, transcendentals=0) if flops else None
    return pl.pallas_call(
        kernel,
        out_shape=out_shape,
        in_specs=specs,
        out_specs=jax.tree.map(lambda _: VM, out_shape),
        scratch_shapes=scratch,
        compiler_params=pltpu.CompilerParams(vmem_limit_bytes=VMEM_LIMIT),
        cost_estimate=cost,
        name=name,
    )(*args)


def per_device(queries, keys, values, w_proj, ln_gain, ln_bias, cotangent):
    tokens_dev, features = queries.shape
    heads, dh, marks = w_proj.shape
    pair = 2 * dh
    width = 4 * dh
    count = tokens_dev * heads
    scale = 1.0 / math.sqrt(dh)
    seqs = lax.axis_size(SEQ)
    sub = lax.axis_size("sub")
    parts = lax.axis_size("part")
    halves = lax.axis_size("half")
    head = lax.axis_index(HEAD).astype(jnp.int32)
    z = lax.axis_index(SEQ).astype(jnp.int32)
    z = z.reshape(1)
    head = head.reshape(1)
    ring = seqs - 1 if 3 <= seqs <= 8 else 0
    wide_part = marks // parts
    tiled = halves == 1 and wide_part == dh and dh % 64 == 0

    packed = call(
        pack_kernel,
        shape_of((heads, tokens_dev, width), BF),
        (z, head, queries, keys, values, cotangent),
        [SM] * 2 + [ANY] * 4,
        "pack",
        [pltpu.VMEM((4, tokens_dev, features), BF), pltpu.SemaphoreType.DMA((4,))],
    )
    x = lax.all_to_all(packed, HEAD, 0, 0, tiled=True).reshape(count, width)

    rows_out = pair + EXTRA
    out_shape = [shape_of((rows_out, marks), BF)]
    if ring:
        out_shape += [shape_of((rows_out, marks + pair), BF)] * 2
    out_shape.append(shape_of((count, marks), BF))
    mid, *halo_outs, expo = call(
        local_sums_kernel, out_shape, (head, x, w_proj), [SM, VM, VM], "local_sums"
    )

    def shifted(block, shift):
        return lax.ppermute(block, SEQ, [(i, (i + shift) % seqs) for i in range(seqs)])

    def forward(block, shift):
        route = [(i, i + shift) for i in range(seqs) if 0 <= i + shift < seqs]
        return lax.ppermute(block, SEQ, route)

    if ring:
        recv = [shifted(halo_outs[0], 1)]
        recv += [shifted(mid, k) for k in range(2, ring)]
        recv += [shifted(halo_outs[1], ring)]
        lands = [mid, *recv]
        halos = [recv[0], recv[-1]]
    else:
        halos = [forward(x[count - WIN :, :pair], 1), forward(x[:WIN, :pair], -1)]
        lands = [lax.all_gather(mid, SEQ), *halos]
    halo_wide = marks + pair if ring else pair
    work = 2 * count * 3 * WIN * pair
    early, a_all, at_all, affine = call(
        functools.partial(window_forward_kernel, scale=scale),
        [
            shape_of((count, 4 * pair), F32),
            shape_of((2 * count, pair), BF),
            shape_of((pair, 2 * count), BF),
            shape_of((2 * pair, pair), F32),
        ],
        (x, ln_gain, ln_bias),
        [VM] * 3,
        "window_forward",
        flops=3 * work,
    )
    late, row_stats, grad_mid, plus, minus, stats = call(
        functools.partial(landmark_forward_kernel, ring=ring, seqs=seqs),
        [
            shape_of((count, pair), F32),
            shape_of((count, 2 * pair), F32),
            shape_of((pair, marks), BF),
            shape_of((pair, halo_wide), BF),
            shape_of((pair, halo_wide), BF),
            shape_of((2 * pair + 8, marks), F32),
        ],
        (z, early, a_all, at_all, *lands, affine),
        [SM] + [VM] * (len(lands) + 4),
        "landmark_forward",
        [pltpu.VMEM((seqs, rows_out, marks), BF)] if ring else [],
    )
    if ring:
        grads = [grad_mid, shifted(plus, 1)]
        grads += [shifted(grad_mid, k) for k in range(2, ring)]
        grads += [shifted(minus, ring)]
    else:
        grads = [lax.all_gather(grad_mid, SEQ), forward(plus, 1), forward(minus, -1)]
    od, dkvt = call(
        functools.partial(window_backward_kernel, scale=scale),
        [shape_of((count, pair), BF), shape_of((pair, count), F32)],
        (x, a_all, at_all, late, row_stats),
        [VM] * 5,
        "window_backward",
        flops=5 * work,
    )
    send_rows = tokens_dev + 8 + (dh // 4 if tiled else 0)
    out_shape = [shape_of((heads, send_rows, width), BF)]
    if not tiled:
        out_shape.append(shape_of((dh, marks), F32))
    send, *proj = call(
        functools.partial(
            final_kernel,
            ring=ring,
            seqs=seqs,
            sub=sub if tiled else 1,
            parts=parts,
            tiled=tiled,
        ),
        out_shape,
        (z, head, *grads, x, w_proj, affine, expo, od, dkvt, stats),
        [SM, SM] + [VM] * (len(grads) + 7),
        "landmark_backward",
        [pltpu.VMEM((seqs, pair, marks), BF)] if ring else [],
    )
    back = lax.all_to_all(send, HEAD, 0, 0, tiled=True)
    out_shape = [shape_of((tokens_dev, features), BF)] * 4 + [shape_of((4, dh), F32)]
    if tiled:
        out_shape.append(shape_of((1, heads, dh, wide_part), F32))
    attended, dq, dk, dv, grad_norm, *tiles = call(
        unpack_kernel, out_shape, (back,), [VM], "unpack", keep=False
    )
    if tiled:
        grad_proj = tiles[0]
    else:
        full = lax.all_gather(proj[0], HEAD)
        inner = ("half", "part") if halves > 1 else "part"
        grad_proj = lax.psum_scatter(full, inner, scatter_dimension=2, tiled=True)[None] / parts
    return (attended, dq, dk, dv, grad_proj, grad_norm)


def solution(mesh):
    ctx, inner = mesh.shape["ctx"], mesh.shape["inner"]

    def whole(queries, keys, values, w_proj, ln_gain, ln_bias, cotangent):
        heads = w_proj.shape[0]
        part = min(heads, inner)
        sub = heads // part
        order = np.asarray(mesh.devices).reshape(ctx // sub, sub, inner // part, part)
        split = Mesh(order, ("seq", "sub", "half", "part"))
        every = P(("seq", "sub", "half", "part"), None)
        return jax.shard_map(
            per_device,
            mesh=split,
            in_specs=(every, every, every, P(), P(), P(), every),
            out_specs=(
                every,
                every,
                every,
                every,
                P(("seq", "sub"), None, None, ("half", "part")),
                P(),
            ),
            check_vma=False,
        )(queries, keys, values, w_proj, ln_gain, ln_bias, cotangent)

    return whole
```

```python
import functools
import math

import jax
import jax.numpy as jnp
import numpy as np
from jax import lax
from jax.experimental import pallas as pl
from jax.experimental.pallas import tpu as pltpu
from jax.sharding import Mesh
from jax.sharding import PartitionSpec as P

WIN = 128
EXTRA = 8
EPS = 1e-05
NEG = -1e30
BATCH = 8
VMEM_LIMIT = 24 * 1024 * 1024
BF = jnp.bfloat16
F32 = jnp.float32

NN = (((1,), (0,)), ((), ()))
NT = (((1,), (1,)), ((), ()))
SEQ = ("seq", "half")
HEAD = ("sub", "part")


def dot(a, b, dims=NN):
    return lax.dot_general(a, b, dims, preferred_element_type=F32)


def lanes(shape):
    return lax.broadcasted_iota(jnp.int32, shape, 1)


def rows(shape):
    return lax.broadcasted_iota(jnp.int32, shape, 0)


def gather_pieces(piece_refs, stack_ref, head):
    for k, ref in enumerate(piece_refs):
        stack_ref[head ^ k] = ref[...]


def scatter_pieces(stack_ref, piece_refs, head):
    for k, ref in enumerate(piece_refs):
        ref[...] = stack_ref[head ^ k]


def pack_kernel(head_ref, z_ref, q_ref, k_ref, v_ref, g_ref, w_src, gain_src, bias_src, *rest):
    *piece_refs, w_ref, gain_ref, bias_ref, stack_ref, buffer_ref, sems = rest
    del z_ref
    heads, _, width = stack_ref.shape
    dh = width // 4
    copies = []
    for slot, ref in enumerate((k_ref, v_ref, q_ref, g_ref)):
        copy = pltpu.make_async_copy(ref, buffer_ref.at[slot], sems.at[slot])
        copy.start()
        copies.append(copy)
    small = ((w_src.at[head_ref[0]], w_ref), (gain_src, gain_ref), (bias_src, bias_ref))
    extra = [
        pltpu.make_async_copy(src, dst, sems.at[len(copies) + slot])
        for slot, (src, dst) in enumerate(small)
    ]
    for copy in extra:
        copy.start()
    for slot, copy in enumerate(copies):
        copy.wait()
        for h in range(heads):
            stack_ref[h, :, slot * dh : (slot + 1) * dh] = buffer_ref[
                slot, :, h * dh : (h + 1) * dh
            ]
    scatter_pieces(stack_ref, piece_refs, head_ref[0])
    for copy in extra:
        copy.wait()


def split_rows(total_rows, width, pieces):
    r = rows((total_rows, width))
    out = jnp.zeros((total_rows, width), F32)
    for index, piece in enumerate(pieces):
        out = jnp.where(r == index, piece, out)
    return out.astype(BF)


def bf_pieces(x, count):
    out = []
    for _ in range(count):
        piece = x.astype(BF).astype(F32)
        out.append(piece)
        x = x - piece
    return out


def widen_proj(w):
    return jnp.concatenate([w, jnp.zeros_like(w)], axis=0)


def local_sums_kernel(head_ref, w_ref, *refs, heads):
    x_ref, expo_ref, mid_ref, *halo_refs = refs[heads:]
    gather_pieces(refs[:heads], x_ref, head_ref[0])
    _, tokens_dev, width = x_ref.shape
    count = heads * tokens_dev
    pair = width // 2
    kv = x_ref[:, :, :pair].reshape(count, pair)
    logits = dot(kv, widen_proj(w_ref[...]))
    peak = jnp.max(logits, axis=0, keepdims=True)
    expo = jnp.exp(logits - peak)
    total = jnp.sum(expo, axis=0, keepdims=True)
    expo_b = expo.astype(BF)
    expo_ref[...] = expo_b
    sums = dot(kv.T, expo_b).astype(BF)
    marks = sums.shape[1]
    tail = split_rows(EXTRA, marks, bf_pieces(peak, 3) + bf_pieces(total, 2))
    targets = [(mid_ref, None)]
    if halo_refs:
        targets += [(halo_refs[0], kv[count - WIN :]), (halo_refs[1], kv[:WIN])]
    for ref, halo in targets:
        ref[:pair, :marks] = sums
        ref[pair:, :marks] = tail
        if halo is not None:
            ref[:pair, marks:] = halo
            ref[pair:, marks:] = jnp.zeros((EXTRA, pair), BF)


def collect(own_ref, recv_refs, stack_ref, index, marks):
    count = len(recv_refs) + 1
    stack_ref[index] = own_ref[...]
    for shift, ref in enumerate(recv_refs, start=1):
        stack_ref[lax.rem(index + (count - shift), count)] = ref[:, :marks]


def as_column(ref):
    row = jnp.concatenate([ref[0:1, :], ref[1:2, :]], axis=1)
    size = row.shape[1]
    return jnp.sum(
        jnp.where(rows((size, size)) == lanes((size, size)), row, 0.0), axis=1, keepdims=True
    )


def spread(x, width):
    return jnp.concatenate([x] * (width // x.shape[1]), axis=1)


def row_max(x):
    return jnp.max(x, axis=1, keepdims=True)


def row_sum(x):
    return jnp.sum(x, axis=1, keepdims=True)


def window_forward_kernel(x_ref, gain_src, bias_src, early_ref, a_ref, at_ref, affine_ref, *, scale):
    count, width = x_ref.shape
    pair = width // 2
    dh = pair // 2
    segments = count // WIN
    low = lanes((WIN, pair)) < dh
    zero_b = jnp.zeros((WIN, pair), BF)
    for slot, src in enumerate((gain_src, bias_src)):
        affine_ref[slot * pair : (slot + 1) * pair] = jnp.broadcast_to(
            as_column(src), (pair, affine_ref.shape[1])
        )
    for s in range(segments):
        qg = x_ref[s * WIN : (s + 1) * WIN, pair:]
        q0 = jnp.where(low, (qg.astype(F32) * scale).astype(BF), zero_b)
        g0 = jnp.where(low, zero_b, qg)
        a = jnp.concatenate([q0, g0], axis=0)
        a_ref[2 * s * WIN : 2 * (s + 1) * WIN] = a
        at_ref[:, 2 * s * WIN : 2 * (s + 1) * WIN] = a.T
        kvw = x_ref[max(s - 1, 0) * WIN : min(s + 2, segments) * WIN, :pair]
        sw = dot(a, kvw, NT)
        scores, grads = sw[:WIN], sw[WIN:]
        top = row_max(scores)
        expo = jnp.exp(scores - top)
        expo_b = expo.astype(BF)
        out = dot(expo_b, kvw)
        part = row_sum(expo * grads)
        span = slice(s * WIN, (s + 1) * WIN)
        early_ref[span, :pair] = out
        for slot, stat in enumerate((top, row_sum(expo), part), start=1):
            early_ref[span, slot * pair : (slot + 1) * pair] = jnp.broadcast_to(stat, out.shape)


def landmark_forward_kernel(*refs, ring, seqs):
    lands = ring + 1 if ring else 3
    z_ref, early_ref, a_ref, at_ref = refs[:4]
    land_refs = refs[4 : 4 + lands]
    affine_ref = refs[4 + lands]
    outs = refs[5 + lands :]
    late_ref, rows_ref, mid_ref, plus_ref, minus_ref, stats_ref, *scratch = outs
    pair = mid_ref.shape[0]
    marks = mid_ref.shape[1]
    dh = pair // 2
    segments = early_ref.shape[0] // WIN
    z = z_ref[0]
    last = seqs - 1
    if ring:
        stack_ref = scratch[0]
        collect(land_refs[0], land_refs[1:], stack_ref, z, marks)
        halos = {0: land_refs[1][:pair, marks:], segments - 1: land_refs[-1][:pair, marks:]}
    else:
        stack_ref = land_refs[0]
        halos = {0: land_refs[1][...], segments - 1: land_refs[2][...]}
    groups = stack_ref.shape[0]

    peaks, totals = [], []
    for j in range(groups):
        tail = stack_ref[j, pair:, :].astype(F32)
        peaks.append(tail[0:1] + tail[1:2] + tail[2:3])
        totals.append(tail[3:4] + tail[4:5])
    peak = functools.reduce(jnp.maximum, peaks)
    total = jnp.zeros_like(peak)
    factors = [jnp.exp(p - peak) for p in peaks]
    for factor, part in zip(factors, totals):
        total = total + factor * part
    inv_total = 1.0 / total
    factors = [factor * inv_total for factor in factors]
    land_t, inverse = [], []
    for half in range(2):
        block = slice(half * dh, (half + 1) * dh)
        mean = factors[0] * stack_ref[0, block, :].astype(F32)
        for j in range(1, groups):
            mean = mean + factors[j] * stack_ref[j, block, :].astype(F32)
        stats_ref[pair + half * dh : pair + (half + 1) * dh] = mean
        centred = mean - jnp.mean(mean, axis=0, keepdims=True)
        inv = 1.0 / jnp.sqrt(jnp.mean(centred * centred, axis=0, keepdims=True) + EPS)
        normed = centred * inv
        stats_ref[block] = normed
        inverse.append(inv)
        gain = affine_ref[half * dh : (half + 1) * dh]
        bias = affine_ref[pair + half * dh : pair + (half + 1) * dh]
        land_t.append((normed * spread(gain, marks) + spread(bias, marks)).astype(BF))
    land_t = jnp.concatenate(land_t, axis=0)
    land = land_t.T
    own_tail = stack_ref[z, pair:, :].astype(F32)
    own_peak = own_tail[0:1] + own_tail[1:2] + own_tail[2:3]
    factor = jnp.exp(own_peak - peak) * inv_total
    r8 = rows((8, marks))
    stats_ref[2 * pair :] = jnp.where(r8 == 0, inverse[0], jnp.where(r8 == 1, inverse[1], factor))

    low = lanes((WIN, pair)) < dh
    land_grad = jnp.zeros((pair, marks), F32)
    halo_grads = {}
    for first in range(0, segments, BATCH):
        batch = range(first, min(first + BATCH, segments))
        spans = {s: slice(s * WIN, (s + 1) * WIN) for s in batch}
        blocks = {s: a_ref[2 * s * WIN : 2 * (s + 1) * WIN] for s in batch}
        early = {
            s: [early_ref[spans[s], slot * pair : (slot + 1) * pair] for slot in range(4)]
            for s in batch
        }
        sl = {s: dot(blocks[s], land_t) for s in batch}
        sh = {s: dot(blocks[s], halos[s], NT) for s in batch if s in halos}
        scores = {s: sl[s][:WIN] for s in batch}
        grads = {s: sl[s][WIN:] for s in batch}
        scores_h = {
            s: jnp.where(z == (0 if s == 0 else last), NEG, sh[s][:WIN]) for s in sh
        }
        top = {s: jnp.maximum(row_max(scores[s]), early[s][1]) for s in batch}
        for s in sh:
            top[s] = jnp.maximum(top[s], row_max(scores_h[s]))
        expo = {s: jnp.exp(scores[s] - spread(top[s], marks)) for s in batch}
        expo_h = {s: jnp.exp(scores_h[s] - top[s]) for s in sh}
        scale_e = {s: jnp.exp(early[s][1] - top[s]) for s in batch}
        total_row, part = {}, {}
        for s in batch:
            total_row[s] = row_sum(expo[s]) + early[s][2] * scale_e[s]
            part[s] = row_sum(expo[s] * grads[s]) + early[s][3] * scale_e[s]
            if s in sh:
                total_row[s] = total_row[s] + row_sum(expo_h[s])
                part[s] = part[s] + row_sum(expo_h[s] * sh[s][WIN:])
        inv = {s: 1.0 / total_row[s] for s in batch}
        delta = {s: part[s] * inv[s] for s in batch}
        b, b_h = {}, {}
        for s in batch:
            probs = expo[s] * spread(inv[s], marks)
            b[s] = jnp.concatenate(
                [(probs * (grads[s] - spread(delta[s], marks))).astype(BF), probs.astype(BF)],
                axis=0,
            )
            rows_ref[spans[s], :pair] = top[s] + jnp.log(total_row[s])
            rows_ref[spans[s], pair:] = delta[s]
        for s in sh:
            probs = expo_h[s] * inv[s]
            b_h[s] = jnp.concatenate(
                [(probs * (sh[s][WIN:] - delta[s])).astype(BF), probs.astype(BF)], axis=0
            )
        for s in batch:
            od = dot(b[s], land)
            if s in sh:
                od = od + dot(b_h[s], halos[s])
            late_ref[spans[s]] = jnp.where(
                low, od[:WIN], od[WIN:] + early[s][0] * (scale_e[s] * inv[s])
            )
        reach = slice(2 * batch[0] * WIN, 2 * (batch[-1] + 1) * WIN)
        land_grad = land_grad + dot(at_ref[:, reach], jnp.concatenate([b[s] for s in batch], axis=0))
        for s in sh:
            halo_grads[s] = dot(at_ref[:, 2 * s * WIN : 2 * (s + 1) * WIN], b_h[s]).astype(BF)
    land_b = land_grad.astype(BF)
    mid_ref[...] = land_b
    if ring:
        plus_ref[:, :marks] = land_b
        minus_ref[:, :marks] = land_b
        plus_ref[:, marks:] = halo_grads[segments - 1]
        minus_ref[:, marks:] = halo_grads[0]
    else:
        plus_ref[...] = halo_grads[segments - 1]
        minus_ref[...] = halo_grads[0]


def window_backward_kernel(x_ref, a_ref, at_ref, late_ref, rows_ref, od_ref, dkvt_ref, *, scale):
    count, width = x_ref.shape
    pair = width // 2
    dh = pair // 2
    segments = count // WIN
    dkvt_ref[...] = jnp.zeros(dkvt_ref.shape, F32)
    low = lanes((WIN, pair)) < dh
    for s in range(segments):
        span = slice(s * WIN, (s + 1) * WIN)
        near = slice(max(s - 1, 0) * WIN, min(s + 2, segments) * WIN)
        a = a_ref[2 * s * WIN : 2 * (s + 1) * WIN]
        kvw = x_ref[near, :pair]
        reach = near.stop - near.start
        sw = dot(a, kvw, NT)
        probs = jnp.exp(sw[:WIN] - spread(rows_ref[span, :pair], reach))
        grad_b = (probs * (sw[WIN:] - spread(rows_ref[span, pair:], reach))).astype(BF)
        late = late_ref[span]
        dq = (dot(grad_b, kvw) + late) * scale
        od_ref[span] = jnp.where(low, dq, late).astype(BF)
        b = jnp.concatenate([grad_b, probs.astype(BF)], axis=0)
        dkvt_ref[:, near] += dot(at_ref[:, 2 * s * WIN : 2 * (s + 1) * WIN], b)


def final_kernel(*refs, ring, seqs, heads, sub, parts, tiled):
    grads_in = ring + 1 if ring else 1
    z_ref, head_ref = refs[:2]
    grad_refs = refs[2 : 2 + grads_in]
    rest = refs[2 + grads_in :]
    if ring:
        prev_src, next_src = grad_refs[1], grad_refs[-1]
    else:
        prev_src, next_src, *rest = rest
    x_ref, w_ref, affine_ref, expo_ref, od_ref, dkvt_ref, stats_ref, *outs = rest
    count, width = x_ref.shape
    pair = width // 2
    dh = pair // 2
    marks = expo_ref.shape[1]
    if ring:
        stack_ref = outs.pop()
        collect(grad_refs[0], grad_refs[1:], stack_ref, z_ref[0], marks)
    else:
        stack_ref = grad_refs[0]
    send_ref = outs.pop()
    piece_refs, proj_refs = outs[:heads], outs[heads:]
    z = z_ref[0]
    from_prev = prev_src[:, prev_src.shape[1] - pair :].astype(F32)
    from_next = next_src[:, next_src.shape[1] - pair :].astype(F32)
    from_prev = jnp.where(z == 0, 0.0, from_prev)
    from_next = jnp.where(z == seqs - 1, 0.0, from_next)
    grad = stack_ref[0].astype(F32)
    for j in range(1, stack_ref.shape[0]):
        grad = grad + stack_ref[j].astype(F32)
    normed = stats_ref[:pair]
    mean = stats_ref[pair : 2 * pair]
    factor = stats_ref[2 * pair + 2 : 2 * pair + 3]
    gained = grad * spread(affine_ref[:pair], marks)
    blocks = []
    for half in range(2):
        part = slice(half * dh, (half + 1) * dh)
        g = gained[part]
        first = jnp.mean(g, axis=0, keepdims=True)
        second = jnp.mean(g * normed[part], axis=0, keepdims=True)
        inv = stats_ref[2 * pair + half : 2 * pair + half + 1]
        blocks.append(inv * (g - first - normed[part] * second))
    grad_mean = jnp.concatenate(blocks, axis=0)
    grad_b = grad_mean.astype(BF)
    column = jnp.sum(grad_b.astype(F32) * mean, axis=0, keepdims=True)
    scaled = (grad_mean * factor).astype(BF)

    gain_sum = jnp.sum(grad * normed, axis=1, keepdims=True)
    bias_sum = jnp.sum(grad, axis=1, keepdims=True)
    lane = lanes((pair, pair))
    square = jnp.where(lane == 0, gain_sum, jnp.where(lane == 1, bias_sum, 0.0)).T
    norm_hi = square[:8].astype(BF)
    norm_lo = (square[:8] - norm_hi.astype(F32)).astype(BF)
    norm_rows = jnp.concatenate(
        [
            jnp.concatenate([norm_hi, norm_lo], axis=1),
        ],
        axis=0,
    )

    kv = x_ref[:, :pair]
    wide = widen_proj(w_ref[...])
    expo_b = expo_ref[...]
    weights = expo_b.astype(F32) * factor
    grad_logit = (weights * (dot(kv, grad_b) - column)).astype(BF)
    land = dot(expo_b, scaled, NT) + dot(grad_logit, wide, NT)
    window = dkvt_ref[...].T
    dests, out_rows, _ = send_ref.shape
    step = count // dests
    dkv = land + window
    head_fix = from_prev.T
    tail_fix = from_next.T
    for d in range(dests):
        span = slice(d * step, (d + 1) * step)
        block = dkv[span]
        fix_top = head_fix if d == 0 else None
        fix_end = tail_fix if d == dests - 1 else None
        for at in range(0, step, WIN):
            piece = block[at : at + WIN]
            if fix_top is not None and at == 0:
                piece = piece + fix_top
            if fix_end is not None and at + WIN == step:
                piece = piece + fix_end
            send_ref[d, at : at + WIN, :pair] = piece.astype(BF)
        send_ref[d, :step, pair:] = od_ref[span]
        send_ref[d, out_rows - 8 :] = norm_rows
    kvt = kv.T
    group = count // sub
    for sb in range(sub):
        span = slice(sb * group, (sb + 1) * group)
        proj = dot(kvt[:, span], grad_logit[span])[:dh]
        if tiled:
            wide_part = marks // parts
            quarter = dh // 4
            for i in range(parts):
                tile = proj[:, i * wide_part : (i + 1) * wide_part].astype(BF)
                for k in range(4):
                    send_ref[
                        sb * parts + i, step : out_rows - 8, k * dh : (k + 1) * dh
                    ] = tile[k * quarter : (k + 1) * quarter]
        else:
            proj_refs[0][...] = proj
    scatter_pieces(send_ref, piece_refs, head_ref[0])


def unpack_kernel(head_ref, *refs, heads):
    att_ref, dq_ref, dk_ref, dv_ref, norm_ref, *proj_refs, r_ref = refs[heads:]
    gather_pieces(refs[:heads], r_ref, head_ref[0])
    heads, _, width = r_ref.shape
    dh = width // 4
    pair = 2 * dh
    step = att_ref.shape[0]
    for h in range(heads):
        cols = slice(h * dh, (h + 1) * dh)
        for slot, ref in enumerate((dk_ref, dv_ref, dq_ref, att_ref)):
            ref[:, cols] = r_ref[h, :step, slot * dh : (slot + 1) * dh]
    norm = jnp.zeros((8, pair), F32)
    for h in range(heads):
        block = r_ref[h, r_ref.shape[1] - 8 :, :].astype(F32)
        norm = norm + (block[:, :pair] + block[:, pair:])
    norm_ref[0:1] = norm[0:1, :dh]
    norm_ref[1:2] = norm[1:2, :dh]
    norm_ref[2:3] = norm[0:1, dh:]
    norm_ref[3:4] = norm[1:2, dh:]
    if proj_refs:
        proj_ref = proj_refs[0]
        quarter = dh // 4
        for h in range(heads):
            for k in range(4):
                proj_ref[0, h, k * quarter : (k + 1) * quarter] = r_ref[
                    h, step : r_ref.shape[1] - 8, k * dh : (k + 1) * dh
                ].astype(F32)


def shape_of(shape, dtype):
    return jax.ShapeDtypeStruct(shape, dtype)


VM = pl.BlockSpec(memory_space=pltpu.VMEM)
SM = pl.BlockSpec(memory_space=pltpu.SMEM)
ANY = pl.BlockSpec(memory_space=pltpu.HBM)


def call(kernel, out_shape, args, specs, name, scratch=(), keep=True, flops=0):
    args = [
        arg if spec is SM else pltpu.with_memory_space_constraint(arg, spec.memory_space)
        for arg, spec in zip(args, specs)
    ]
    if keep:
        out_shape = jax.tree.map(lambda s: pltpu.VMEM(s.shape, s.dtype), out_shape)
    cost = pl.CostEstimate(flops=flops, bytes_accessed=0, transcendentals=0) if flops else None
    return pl.pallas_call(
        kernel,
        out_shape=out_shape,
        in_specs=specs,
        out_specs=jax.tree.map(lambda _: VM, out_shape),
        scratch_shapes=scratch,
        compiler_params=pltpu.CompilerParams(vmem_limit_bytes=VMEM_LIMIT),
        cost_estimate=cost,
        name=name,
    )(*args)


def per_device(queries, keys, values, w_proj, ln_gain, ln_bias, cotangent):
    tokens_dev, features = queries.shape
    heads, dh, marks = w_proj.shape
    pair = 2 * dh
    width = 4 * dh
    count = tokens_dev * heads
    scale = 1.0 / math.sqrt(dh)
    seqs = lax.axis_size(SEQ)
    sub = lax.axis_size("sub")
    parts = lax.axis_size("part")
    halves = lax.axis_size("half")
    head = lax.axis_index(HEAD).astype(jnp.int32)
    z = lax.axis_index(SEQ).astype(jnp.int32)
    z = z.reshape(1)
    head = head.reshape(1)
    ring = seqs - 1 if 3 <= seqs <= 8 else 0
    wide_part = marks // parts
    tiled = halves == 1 and wide_part == dh and dh % 64 == 0

    def exchange(pieces):
        out = dict(enumerate(pieces[:1]))
        for k in reversed(range(1, heads)):
            out[k] = lax.ppermute(pieces[k], HEAD, [(i, i ^ k) for i in range(heads)])
        return [out[k] for k in range(heads)]

    *packed, w_head, gain, bias = call(
        pack_kernel,
        [shape_of((tokens_dev, width), BF)] * heads
        + [shape_of((dh, marks), BF)]
        + [shape_of((2, dh), F32)] * 2,
        (head, z, queries, keys, values, cotangent, w_proj, ln_gain, ln_bias),
        [SM] * 2 + [ANY] * 7,
        "pack",
        [
            pltpu.VMEM((heads, tokens_dev, width), BF),
            pltpu.VMEM((4, tokens_dev, features), BF),
            pltpu.SemaphoreType.DMA((7,)),
        ],
    )
    pieces = exchange(packed)

    rows_out = pair + EXTRA
    out_shape = [
        shape_of((heads, tokens_dev, width), BF),
        shape_of((count, marks), BF),
        shape_of((rows_out, marks), BF),
    ]
    if ring:
        out_shape += [shape_of((rows_out, marks + pair), BF)] * 2
    x, expo, mid, *halo_outs = call(
        functools.partial(local_sums_kernel, heads=heads),
        out_shape,
        (head, w_head, *pieces),
        [SM] + [VM] * (heads + 1),
        "local_sums",
    )
    x = x.reshape(count, width)

    def shifted(block, shift):
        return lax.ppermute(block, SEQ, [(i, (i + shift) % seqs) for i in range(seqs)])

    def forward(block, shift):
        route = [(i, i + shift) for i in range(seqs) if 0 <= i + shift < seqs]
        return lax.ppermute(block, SEQ, route)

    if ring:
        recv = [shifted(halo_outs[0], 1)]
        recv += [shifted(mid, k) for k in range(2, ring)]
        recv += [shifted(halo_outs[1], ring)]
        lands = [mid, *recv]
        halos = [recv[0], recv[-1]]
    else:
        halos = [forward(x[count - WIN :, :pair], 1), forward(x[:WIN, :pair], -1)]
        lands = [lax.all_gather(mid, SEQ), *halos]
    halo_wide = marks + pair if ring else pair
    work = 2 * count * 3 * WIN * pair
    early, a_all, at_all, affine = call(
        functools.partial(window_forward_kernel, scale=scale),
        [
            shape_of((count, 4 * pair), F32),
            shape_of((2 * count, pair), BF),
            shape_of((pair, 2 * count), BF),
            shape_of((2 * pair, pair), F32),
        ],
        (x, gain, bias),
        [VM] * 3,
        "window_forward",
        flops=3 * work,
    )
    late, row_stats, grad_mid, plus, minus, stats = call(
        functools.partial(landmark_forward_kernel, ring=ring, seqs=seqs),
        [
            shape_of((count, pair), F32),
            shape_of((count, 2 * pair), F32),
            shape_of((pair, marks), BF),
            shape_of((pair, halo_wide), BF),
            shape_of((pair, halo_wide), BF),
            shape_of((2 * pair + 8, marks), F32),
        ],
        (z, early, a_all, at_all, *lands, affine),
        [SM] + [VM] * (len(lands) + 4),
        "landmark_forward",
        [pltpu.VMEM((seqs, rows_out, marks), BF)] if ring else [],
    )
    if ring:
        grads = [grad_mid, shifted(plus, 1)]
        grads += [shifted(grad_mid, k) for k in range(2, ring)]
        grads += [shifted(minus, ring)]
    else:
        grads = [lax.all_gather(grad_mid, SEQ), forward(plus, 1), forward(minus, -1)]
    od, dkvt = call(
        functools.partial(window_backward_kernel, scale=scale),
        [shape_of((count, pair), BF), shape_of((pair, count), F32)],
        (x, a_all, at_all, late, row_stats),
        [VM] * 5,
        "window_backward",
        flops=5 * work,
    )
    send_rows = tokens_dev + 8 + (dh // 4 if tiled else 0)
    out_shape = [shape_of((send_rows, width), BF)] * heads
    if not tiled:
        out_shape.append(shape_of((dh, marks), F32))
    sent = call(
        functools.partial(
            final_kernel,
            ring=ring,
            seqs=seqs,
            heads=heads,
            sub=sub if tiled else 1,
            parts=parts,
            tiled=tiled,
        ),
        out_shape,
        (z, head, *grads, x, w_head, affine, expo, od, dkvt, stats),
        [SM, SM] + [VM] * (len(grads) + 7),
        "landmark_backward",
        [pltpu.VMEM((heads, send_rows, width), BF)]
        + ([pltpu.VMEM((seqs, pair, marks), BF)] if ring else []),
    )
    back = exchange(sent[:heads])
    out_shape = [shape_of((tokens_dev, features), BF)] * 4 + [shape_of((4, dh), F32)]
    if tiled:
        out_shape.append(shape_of((1, heads, dh, wide_part), F32))
    attended, dq, dk, dv, grad_norm, *tiles = call(
        functools.partial(unpack_kernel, heads=heads),
        out_shape,
        (head, *back),
        [SM] + [VM] * heads,
        "unpack",
        [pltpu.VMEM((heads, send_rows, width), BF)],
        keep=False,
    )
    if tiled:
        grad_proj = tiles[0]
    else:
        full = lax.all_gather(sent[-1], HEAD)
        inner = ("half", "part") if halves > 1 else "part"
        grad_proj = lax.psum_scatter(full, inner, scatter_dimension=2, tiled=True)[None] / parts
    return (attended, dq, dk, dv, grad_proj, grad_norm)


def solution(mesh):
    ctx, inner = mesh.shape["ctx"], mesh.shape["inner"]

    def whole(queries, keys, values, w_proj, ln_gain, ln_bias, cotangent):
        heads = w_proj.shape[0]
        part = min(heads, inner)
        sub = heads // part
        order = np.asarray(mesh.devices).reshape(ctx // sub, sub, inner // part, part)
        split = Mesh(order, ("seq", "sub", "half", "part"))
        every = P(("seq", "sub", "half", "part"), None)
        return jax.shard_map(
            per_device,
            mesh=split,
            in_specs=(every, every, every, P(), P(), P(), every),
            out_specs=(
                every,
                every,
                every,
                every,
                P(("seq", "sub"), None, None, ("half", "part")),
                P(),
            ),
            check_vma=False,
        )(queries, keys, values, w_proj, ln_gain, ln_bias, cotangent)

    return whole
```

```python
import functools
import math

import jax
import jax.numpy as jnp
import numpy as np
from jax import lax
from jax.experimental import pallas as pl
from jax.experimental.pallas import tpu as pltpu
from jax.sharding import Mesh
from jax.sharding import PartitionSpec as P

WIN = 128
EXTRA = 8
EPS = 1e-05
NEG = -1e30
BATCH = 8
VMEM_LIMIT = 24 * 1024 * 1024
BF = jnp.bfloat16
F32 = jnp.float32

NN = (((1,), (0,)), ((), ()))
NT = (((1,), (1,)), ((), ()))
SEQ = ("seq", "half")
HEAD = ("sub", "part")


def dot(a, b, dims=NN):
    return lax.dot_general(a, b, dims, preferred_element_type=F32)


def lanes(shape):
    return lax.broadcasted_iota(jnp.int32, shape, 1)


def rows(shape):
    return lax.broadcasted_iota(jnp.int32, shape, 0)


def peer_order(heads):
    return [0, 7, 4, 2, 6, 5, 3, 1]


def gather_pieces(piece_refs, stack_ref, head):
    for k, ref in zip(peer_order(len(piece_refs)), piece_refs):
        stack_ref[head ^ k] = ref[...]


def scatter_pieces(stack_ref, piece_refs, head):
    for k, ref in zip(peer_order(len(piece_refs)), piece_refs):
        ref[...] = stack_ref[head ^ k]


def pack_kernel(head_ref, z_ref, q_ref, k_ref, v_ref, g_ref, w_src, gain_src, bias_src, *rest):
    *piece_refs, w_ref, gain_ref, bias_ref, stack_ref, buffer_ref, sems = rest
    del z_ref
    heads, _, width = stack_ref.shape
    dh = width // 4
    copies = []
    for slot, ref in enumerate((k_ref, v_ref, q_ref, g_ref)):
        copy = pltpu.make_async_copy(ref, buffer_ref.at[slot], sems.at[slot])
        copy.start()
        copies.append(copy)
    small = ((w_src.at[head_ref[0]], w_ref), (gain_src, gain_ref), (bias_src, bias_ref))
    extra = [
        pltpu.make_async_copy(src, dst, sems.at[len(copies) + slot])
        for slot, (src, dst) in enumerate(small)
    ]
    for copy in extra:
        copy.start()
    for slot, copy in enumerate(copies):
        copy.wait()
        for h in range(heads):
            stack_ref[h, :, slot * dh : (slot + 1) * dh] = buffer_ref[
                slot, :, h * dh : (h + 1) * dh
            ]
    scatter_pieces(stack_ref, piece_refs, head_ref[0])
    for copy in extra:
        copy.wait()


def split_rows(total_rows, width, pieces):
    r = rows((total_rows, width))
    out = jnp.zeros((total_rows, width), F32)
    for index, piece in enumerate(pieces):
        out = jnp.where(r == index, piece, out)
    return out.astype(BF)


def bf_pieces(x, count):
    out = []
    for _ in range(count):
        piece = x.astype(BF).astype(F32)
        out.append(piece)
        x = x - piece
    return out


def widen_proj(w):
    return jnp.concatenate([w, jnp.zeros_like(w)], axis=0)


def local_sums_kernel(head_ref, w_ref, *refs, heads):
    x_ref, expo_ref, mid_ref, *halo_refs = refs[heads:]
    gather_pieces(refs[:heads], x_ref, head_ref[0])
    _, tokens_dev, width = x_ref.shape
    count = heads * tokens_dev
    pair = width // 2
    kv = x_ref[:, :, :pair].reshape(count, pair)
    logits = dot(kv, widen_proj(w_ref[...]))
    peak = jnp.max(logits, axis=0, keepdims=True)
    expo = jnp.exp(logits - peak)
    total = jnp.sum(expo, axis=0, keepdims=True)
    expo_b = expo.astype(BF)
    expo_ref[...] = expo_b
    sums = dot(kv.T, expo_b).astype(BF)
    marks = sums.shape[1]
    tail = split_rows(EXTRA, marks, bf_pieces(peak, 3) + bf_pieces(total, 2))
    targets = [(mid_ref, None)]
    if halo_refs:
        targets += [(halo_refs[0], kv[count - WIN :]), (halo_refs[1], kv[:WIN])]
    for ref, halo in targets:
        ref[:pair, :marks] = sums
        ref[pair:, :marks] = tail
        if halo is not None:
            ref[:pair, marks:] = halo
            ref[pair:, marks:] = jnp.zeros((EXTRA, pair), BF)


def collect(own_ref, recv_refs, stack_ref, index, marks):
    count = len(recv_refs) + 1
    stack_ref[index] = own_ref[...]
    for shift, ref in enumerate(recv_refs, start=1):
        stack_ref[lax.rem(index + (count - shift), count)] = ref[:, :marks]


def as_column(ref):
    row = jnp.concatenate([ref[0:1, :], ref[1:2, :]], axis=1)
    size = row.shape[1]
    return jnp.sum(
        jnp.where(rows((size, size)) == lanes((size, size)), row, 0.0), axis=1, keepdims=True
    )


def spread(x, width):
    return jnp.concatenate([x] * (width // x.shape[1]), axis=1)


def row_max(x):
    return jnp.max(x, axis=1, keepdims=True)


def row_sum(x):
    return jnp.sum(x, axis=1, keepdims=True)


def window_forward_kernel(x_ref, gain_src, bias_src, early_ref, a_ref, at_ref, affine_ref, *, scale):
    count, width = x_ref.shape
    pair = width // 2
    dh = pair // 2
    segments = count // WIN
    low = lanes((WIN, pair)) < dh
    zero_b = jnp.zeros((WIN, pair), BF)
    for slot, src in enumerate((gain_src, bias_src)):
        affine_ref[slot * pair : (slot + 1) * pair] = jnp.broadcast_to(
            as_column(src), (pair, affine_ref.shape[1])
        )
    for s in range(segments):
        qg = x_ref[s * WIN : (s + 1) * WIN, pair:]
        q0 = jnp.where(low, (qg.astype(F32) * scale).astype(BF), zero_b)
        g0 = jnp.where(low, zero_b, qg)
        a = jnp.concatenate([q0, g0], axis=0)
        a_ref[2 * s * WIN : 2 * (s + 1) * WIN] = a
        at_ref[:, 2 * s * WIN : 2 * (s + 1) * WIN] = a.T
        kvw = x_ref[max(s - 1, 0) * WIN : min(s + 2, segments) * WIN, :pair]
        sw = dot(a, kvw, NT)
        scores, grads = sw[:WIN], sw[WIN:]
        top = row_max(scores)
        expo = jnp.exp(scores - top)
        expo_b = expo.astype(BF)
        out = dot(expo_b, kvw)
        part = row_sum(expo * grads)
        span = slice(s * WIN, (s + 1) * WIN)
        early_ref[span, :pair] = out
        for slot, stat in enumerate((top, row_sum(expo), part), start=1):
            early_ref[span, slot * pair : (slot + 1) * pair] = jnp.broadcast_to(stat, out.shape)


def landmark_forward_kernel(*refs, ring, seqs):
    lands = ring + 1 if ring else 3
    z_ref, early_ref, a_ref, at_ref = refs[:4]
    land_refs = refs[4 : 4 + lands]
    affine_ref = refs[4 + lands]
    outs = refs[5 + lands :]
    late_ref, rows_ref, mid_ref, plus_ref, minus_ref, stats_ref, *scratch = outs
    pair = mid_ref.shape[0]
    marks = mid_ref.shape[1]
    dh = pair // 2
    segments = early_ref.shape[0] // WIN
    z = z_ref[0]
    last = seqs - 1
    if ring:
        stack_ref = scratch[0]
        collect(land_refs[0], land_refs[1:], stack_ref, z, marks)
        halos = {0: land_refs[1][:pair, marks:], segments - 1: land_refs[-1][:pair, marks:]}
    else:
        stack_ref = land_refs[0]
        halos = {0: land_refs[1][...], segments - 1: land_refs[2][...]}
    groups = stack_ref.shape[0]

    peaks, totals = [], []
    for j in range(groups):
        tail = stack_ref[j, pair:, :].astype(F32)
        peaks.append(tail[0:1] + tail[1:2] + tail[2:3])
        totals.append(tail[3:4] + tail[4:5])
    peak = functools.reduce(jnp.maximum, peaks)
    total = jnp.zeros_like(peak)
    factors = [jnp.exp(p - peak) for p in peaks]
    for factor, part in zip(factors, totals):
        total = total + factor * part
    inv_total = 1.0 / total
    factors = [factor * inv_total for factor in factors]
    land_t, inverse = [], []
    for half in range(2):
        block = slice(half * dh, (half + 1) * dh)
        mean = factors[0] * stack_ref[0, block, :].astype(F32)
        for j in range(1, groups):
            mean = mean + factors[j] * stack_ref[j, block, :].astype(F32)
        stats_ref[pair + half * dh : pair + (half + 1) * dh] = mean
        centred = mean - jnp.mean(mean, axis=0, keepdims=True)
        inv = 1.0 / jnp.sqrt(jnp.mean(centred * centred, axis=0, keepdims=True) + EPS)
        normed = centred * inv
        stats_ref[block] = normed
        inverse.append(inv)
        gain = affine_ref[half * dh : (half + 1) * dh]
        bias = affine_ref[pair + half * dh : pair + (half + 1) * dh]
        land_t.append((normed * spread(gain, marks) + spread(bias, marks)).astype(BF))
    land_t = jnp.concatenate(land_t, axis=0)
    land = land_t.T
    own_tail = stack_ref[z, pair:, :].astype(F32)
    own_peak = own_tail[0:1] + own_tail[1:2] + own_tail[2:3]
    factor = jnp.exp(own_peak - peak) * inv_total
    r8 = rows((8, marks))
    stats_ref[2 * pair :] = jnp.where(r8 == 0, inverse[0], jnp.where(r8 == 1, inverse[1], factor))

    low = lanes((WIN, pair)) < dh
    land_grad = jnp.zeros((pair, marks), F32)
    halo_grads = {}
    for first in range(0, segments, BATCH):
        batch = range(first, min(first + BATCH, segments))
        spans = {s: slice(s * WIN, (s + 1) * WIN) for s in batch}
        blocks = {s: a_ref[2 * s * WIN : 2 * (s + 1) * WIN] for s in batch}
        early = {
            s: [early_ref[spans[s], slot * pair : (slot + 1) * pair] for slot in range(4)]
            for s in batch
        }
        sl = {s: dot(blocks[s], land_t) for s in batch}
        sh = {s: dot(blocks[s], halos[s], NT) for s in batch if s in halos}
        scores = {s: sl[s][:WIN] for s in batch}
        grads = {s: sl[s][WIN:] for s in batch}
        scores_h = {
            s: jnp.where(z == (0 if s == 0 else last), NEG, sh[s][:WIN]) for s in sh
        }
        top = {s: jnp.maximum(row_max(scores[s]), early[s][1]) for s in batch}
        for s in sh:
            top[s] = jnp.maximum(top[s], row_max(scores_h[s]))
        expo = {s: jnp.exp(scores[s] - spread(top[s], marks)) for s in batch}
        expo_h = {s: jnp.exp(scores_h[s] - top[s]) for s in sh}
        scale_e = {s: jnp.exp(early[s][1] - top[s]) for s in batch}
        total_row, part = {}, {}
        for s in batch:
            total_row[s] = row_sum(expo[s]) + early[s][2] * scale_e[s]
            part[s] = row_sum(expo[s] * grads[s]) + early[s][3] * scale_e[s]
            if s in sh:
                total_row[s] = total_row[s] + row_sum(expo_h[s])
                part[s] = part[s] + row_sum(expo_h[s] * sh[s][WIN:])
        inv = {s: 1.0 / total_row[s] for s in batch}
        delta = {s: part[s] * inv[s] for s in batch}
        b, b_h = {}, {}
        for s in batch:
            probs = expo[s] * spread(inv[s], marks)
            b[s] = jnp.concatenate(
                [(probs * (grads[s] - spread(delta[s], marks))).astype(BF), probs.astype(BF)],
                axis=0,
            )
            rows_ref[spans[s], :pair] = top[s] + jnp.log(total_row[s])
            rows_ref[spans[s], pair:] = delta[s]
        for s in sh:
            probs = expo_h[s] * inv[s]
            b_h[s] = jnp.concatenate(
                [(probs * (sh[s][WIN:] - delta[s])).astype(BF), probs.astype(BF)], axis=0
            )
        for s in batch:
            od = dot(b[s], land)
            if s in sh:
                od = od + dot(b_h[s], halos[s])
            late_ref[spans[s]] = jnp.where(
                low, od[:WIN], od[WIN:] + early[s][0] * (scale_e[s] * inv[s])
            )
        reach = slice(2 * batch[0] * WIN, 2 * (batch[-1] + 1) * WIN)
        land_grad = land_grad + dot(at_ref[:, reach], jnp.concatenate([b[s] for s in batch], axis=0))
        for s in sh:
            halo_grads[s] = dot(at_ref[:, 2 * s * WIN : 2 * (s + 1) * WIN], b_h[s]).astype(BF)
    land_b = land_grad.astype(BF)
    mid_ref[...] = land_b
    if ring:
        plus_ref[:, :marks] = land_b
        minus_ref[:, :marks] = land_b
        plus_ref[:, marks:] = halo_grads[segments - 1]
        minus_ref[:, marks:] = halo_grads[0]
    else:
        plus_ref[...] = halo_grads[segments - 1]
        minus_ref[...] = halo_grads[0]


def window_backward_kernel(x_ref, a_ref, at_ref, late_ref, rows_ref, od_ref, dkvt_ref, *, scale):
    count, width = x_ref.shape
    pair = width // 2
    dh = pair // 2
    segments = count // WIN
    dkvt_ref[...] = jnp.zeros(dkvt_ref.shape, F32)
    low = lanes((WIN, pair)) < dh
    for s in range(segments):
        span = slice(s * WIN, (s + 1) * WIN)
        near = slice(max(s - 1, 0) * WIN, min(s + 2, segments) * WIN)
        a = a_ref[2 * s * WIN : 2 * (s + 1) * WIN]
        kvw = x_ref[near, :pair]
        reach = near.stop - near.start
        sw = dot(a, kvw, NT)
        probs = jnp.exp(sw[:WIN] - spread(rows_ref[span, :pair], reach))
        grad_b = (probs * (sw[WIN:] - spread(rows_ref[span, pair:], reach))).astype(BF)
        late = late_ref[span]
        dq = (dot(grad_b, kvw) + late) * scale
        od_ref[span] = jnp.where(low, dq, late).astype(BF)
        b = jnp.concatenate([grad_b, probs.astype(BF)], axis=0)
        dkvt_ref[:, near] += dot(at_ref[:, 2 * s * WIN : 2 * (s + 1) * WIN], b)


def final_kernel(*refs, ring, seqs, heads, sub, parts, tiled):
    grads_in = ring + 1 if ring else 1
    z_ref, head_ref = refs[:2]
    grad_refs = refs[2 : 2 + grads_in]
    rest = refs[2 + grads_in :]
    if ring:
        prev_src, next_src = grad_refs[1], grad_refs[-1]
    else:
        prev_src, next_src, *rest = rest
    x_ref, w_ref, affine_ref, expo_ref, od_ref, dkvt_ref, stats_ref, *outs = rest
    count, width = x_ref.shape
    pair = width // 2
    dh = pair // 2
    marks = expo_ref.shape[1]
    if ring:
        stack_ref = outs.pop()
        collect(grad_refs[0], grad_refs[1:], stack_ref, z_ref[0], marks)
    else:
        stack_ref = grad_refs[0]
    send_ref = outs.pop()
    piece_refs, proj_refs = outs[:heads], outs[heads:]
    z = z_ref[0]
    from_prev = prev_src[:, prev_src.shape[1] - pair :].astype(F32)
    from_next = next_src[:, next_src.shape[1] - pair :].astype(F32)
    from_prev = jnp.where(z == 0, 0.0, from_prev)
    from_next = jnp.where(z == seqs - 1, 0.0, from_next)
    grad = stack_ref[0].astype(F32)
    for j in range(1, stack_ref.shape[0]):
        grad = grad + stack_ref[j].astype(F32)
    normed = stats_ref[:pair]
    mean = stats_ref[pair : 2 * pair]
    factor = stats_ref[2 * pair + 2 : 2 * pair + 3]
    gained = grad * spread(affine_ref[:pair], marks)
    blocks = []
    for half in range(2):
        part = slice(half * dh, (half + 1) * dh)
        g = gained[part]
        first = jnp.mean(g, axis=0, keepdims=True)
        second = jnp.mean(g * normed[part], axis=0, keepdims=True)
        inv = stats_ref[2 * pair + half : 2 * pair + half + 1]
        blocks.append(inv * (g - first - normed[part] * second))
    grad_mean = jnp.concatenate(blocks, axis=0)
    grad_b = grad_mean.astype(BF)
    column = jnp.sum(grad_b.astype(F32) * mean, axis=0, keepdims=True)
    scaled = (grad_mean * factor).astype(BF)

    gain_sum = jnp.sum(grad * normed, axis=1, keepdims=True)
    bias_sum = jnp.sum(grad, axis=1, keepdims=True)
    lane = lanes((pair, pair))
    square = jnp.where(lane == 0, gain_sum, jnp.where(lane == 1, bias_sum, 0.0)).T
    norm_hi = square[:8].astype(BF)
    norm_lo = (square[:8] - norm_hi.astype(F32)).astype(BF)
    norm_rows = jnp.concatenate(
        [
            jnp.concatenate([norm_hi, norm_lo], axis=1),
        ],
        axis=0,
    )

    kv = x_ref[:, :pair]
    wide = widen_proj(w_ref[...])
    expo_b = expo_ref[...]
    weights = expo_b.astype(F32) * factor
    grad_logit = (weights * (dot(kv, grad_b) - column)).astype(BF)
    land = dot(expo_b, scaled, NT) + dot(grad_logit, wide, NT)
    window = dkvt_ref[...].T
    dests, out_rows, _ = send_ref.shape
    step = count // dests
    dkv = land + window
    head_fix = from_prev.T
    tail_fix = from_next.T
    for d in range(dests):
        span = slice(d * step, (d + 1) * step)
        block = dkv[span]
        fix_top = head_fix if d == 0 else None
        fix_end = tail_fix if d == dests - 1 else None
        for at in range(0, step, WIN):
            piece = block[at : at + WIN]
            if fix_top is not None and at == 0:
                piece = piece + fix_top
            if fix_end is not None and at + WIN == step:
                piece = piece + fix_end
            send_ref[d, at : at + WIN, :pair] = piece.astype(BF)
        send_ref[d, :step, pair:] = od_ref[span]
        send_ref[d, out_rows - 8 :] = norm_rows
    kvt = kv.T
    group = count // sub
    for sb in range(sub):
        span = slice(sb * group, (sb + 1) * group)
        proj = dot(kvt[:, span], grad_logit[span])[:dh]
        if tiled:
            wide_part = marks // parts
            quarter = dh // 4
            for i in range(parts):
                tile = proj[:, i * wide_part : (i + 1) * wide_part].astype(BF)
                for k in range(4):
                    send_ref[
                        sb * parts + i, step : out_rows - 8, k * dh : (k + 1) * dh
                    ] = tile[k * quarter : (k + 1) * quarter]
        else:
            proj_refs[0][...] = proj
    scatter_pieces(send_ref, piece_refs, head_ref[0])


def unpack_kernel(head_ref, *refs, heads):
    att_ref, dq_ref, dk_ref, dv_ref, norm_ref, *proj_refs, r_ref = refs[heads:]
    gather_pieces(refs[:heads], r_ref, head_ref[0])
    heads, _, width = r_ref.shape
    dh = width // 4
    pair = 2 * dh
    step = att_ref.shape[0]
    for h in range(heads):
        cols = slice(h * dh, (h + 1) * dh)
        for slot, ref in enumerate((dk_ref, dv_ref, dq_ref, att_ref)):
            ref[:, cols] = r_ref[h, :step, slot * dh : (slot + 1) * dh]
    norm = jnp.zeros((8, pair), F32)
    for h in range(heads):
        block = r_ref[h, r_ref.shape[1] - 8 :, :].astype(F32)
        norm = norm + (block[:, :pair] + block[:, pair:])
    norm_ref[0:1] = norm[0:1, :dh]
    norm_ref[1:2] = norm[1:2, :dh]
    norm_ref[2:3] = norm[0:1, dh:]
    norm_ref[3:4] = norm[1:2, dh:]
    if proj_refs:
        proj_ref = proj_refs[0]
        quarter = dh // 4
        for h in range(heads):
            for k in range(4):
                proj_ref[0, h, k * quarter : (k + 1) * quarter] = r_ref[
                    h, step : r_ref.shape[1] - 8, k * dh : (k + 1) * dh
                ].astype(F32)


def shape_of(shape, dtype):
    return jax.ShapeDtypeStruct(shape, dtype)


VM = pl.BlockSpec(memory_space=pltpu.VMEM)
SM = pl.BlockSpec(memory_space=pltpu.SMEM)
ANY = pl.BlockSpec(memory_space=pltpu.HBM)


def call(kernel, out_shape, args, specs, name, scratch=(), keep=True, flops=0):
    args = [
        arg if spec is SM else pltpu.with_memory_space_constraint(arg, spec.memory_space)
        for arg, spec in zip(args, specs)
    ]
    if keep:
        out_shape = jax.tree.map(lambda s: pltpu.VMEM(s.shape, s.dtype), out_shape)
    cost = pl.CostEstimate(flops=flops, bytes_accessed=0, transcendentals=0) if flops else None
    return pl.pallas_call(
        kernel,
        out_shape=out_shape,
        in_specs=specs,
        out_specs=jax.tree.map(lambda _: VM, out_shape),
        scratch_shapes=scratch,
        compiler_params=pltpu.CompilerParams(vmem_limit_bytes=VMEM_LIMIT),
        cost_estimate=cost,
        name=name,
    )(*args)


def per_device(queries, keys, values, w_proj, ln_gain, ln_bias, cotangent):
    tokens_dev, features = queries.shape
    heads, dh, marks = w_proj.shape
    pair = 2 * dh
    width = 4 * dh
    count = tokens_dev * heads
    scale = 1.0 / math.sqrt(dh)
    seqs = lax.axis_size(SEQ)
    sub = lax.axis_size("sub")
    parts = lax.axis_size("part")
    halves = lax.axis_size("half")
    head = lax.axis_index(HEAD).astype(jnp.int32)
    z = lax.axis_index(SEQ).astype(jnp.int32)
    z = z.reshape(1)
    head = head.reshape(1)
    ring = seqs - 1 if 3 <= seqs <= 8 else 0
    wide_part = marks // parts
    tiled = halves == 1 and wide_part == dh and dh % 64 == 0

    def exchange(pieces):
        return [pieces[0]] + [
            lax.ppermute(piece, HEAD, [(i, i ^ k) for i in range(heads)])
            for k, piece in zip(peer_order(heads)[1:], pieces[1:])
        ]

    *packed, w_head, gain, bias = call(
        pack_kernel,
        [shape_of((tokens_dev, width), BF)] * heads
        + [shape_of((dh, marks), BF)]
        + [shape_of((2, dh), F32)] * 2,
        (head, z, queries, keys, values, cotangent, w_proj, ln_gain, ln_bias),
        [SM] * 2 + [ANY] * 7,
        "pack",
        [
            pltpu.VMEM((heads, tokens_dev, width), BF),
            pltpu.VMEM((4, tokens_dev, features), BF),
            pltpu.SemaphoreType.DMA((7,)),
        ],
    )
    pieces = exchange(packed)

    rows_out = pair + EXTRA
    out_shape = [
        shape_of((heads, tokens_dev, width), BF),
        shape_of((count, marks), BF),
        shape_of((rows_out, marks), BF),
    ]
    if ring:
        out_shape += [shape_of((rows_out, marks + pair), BF)] * 2
    x, expo, mid, *halo_outs = call(
        functools.partial(local_sums_kernel, heads=heads),
        out_shape,
        (head, w_head, *pieces),
        [SM] + [VM] * (heads + 1),
        "local_sums",
    )
    x = x.reshape(count, width)

    def shifted(block, shift):
        return lax.ppermute(block, SEQ, [(i, (i + shift) % seqs) for i in range(seqs)])

    def forward(block, shift):
        route = [(i, i + shift) for i in range(seqs) if 0 <= i + shift < seqs]
        return lax.ppermute(block, SEQ, route)

    if ring:
        recv = [shifted(halo_outs[0], 1)]
        recv += [shifted(mid, k) for k in range(2, ring)]
        recv += [shifted(halo_outs[1], ring)]
        lands = [mid, *recv]
        halos = [recv[0], recv[-1]]
    else:
        halos = [forward(x[count - WIN :, :pair], 1), forward(x[:WIN, :pair], -1)]
        lands = [lax.all_gather(mid, SEQ), *halos]
    halo_wide = marks + pair if ring else pair
    work = 2 * count * 3 * WIN * pair
    early, a_all, at_all, affine = call(
        functools.partial(window_forward_kernel, scale=scale),
        [
            shape_of((count, 4 * pair), F32),
            shape_of((2 * count, pair), BF),
            shape_of((pair, 2 * count), BF),
            shape_of((2 * pair, pair), F32),
        ],
        (x, gain, bias),
        [VM] * 3,
        "window_forward",
        flops=3 * work,
    )
    late, row_stats, grad_mid, plus, minus, stats = call(
        functools.partial(landmark_forward_kernel, ring=ring, seqs=seqs),
        [
            shape_of((count, pair), F32),
            shape_of((count, 2 * pair), F32),
            shape_of((pair, marks), BF),
            shape_of((pair, halo_wide), BF),
            shape_of((pair, halo_wide), BF),
            shape_of((2 * pair + 8, marks), F32),
        ],
        (z, early, a_all, at_all, *lands, affine),
        [SM] + [VM] * (len(lands) + 4),
        "landmark_forward",
        [pltpu.VMEM((seqs, rows_out, marks), BF)] if ring else [],
    )
    if ring:
        grads = [grad_mid, shifted(plus, 1)]
        grads += [shifted(grad_mid, k) for k in range(2, ring)]
        grads += [shifted(minus, ring)]
    else:
        grads = [lax.all_gather(grad_mid, SEQ), forward(plus, 1), forward(minus, -1)]
    od, dkvt = call(
        functools.partial(window_backward_kernel, scale=scale),
        [shape_of((count, pair), BF), shape_of((pair, count), F32)],
        (x, a_all, at_all, late, row_stats),
        [VM] * 5,
        "window_backward",
        flops=5 * work,
    )
    send_rows = tokens_dev + 8 + (dh // 4 if tiled else 0)
    out_shape = [shape_of((send_rows, width), BF)] * heads
    if not tiled:
        out_shape.append(shape_of((dh, marks), F32))
    sent = call(
        functools.partial(
            final_kernel,
            ring=ring,
            seqs=seqs,
            heads=heads,
            sub=sub if tiled else 1,
            parts=parts,
            tiled=tiled,
        ),
        out_shape,
        (z, head, *grads, x, w_head, affine, expo, od, dkvt, stats),
        [SM, SM] + [VM] * (len(grads) + 7),
        "landmark_backward",
        [pltpu.VMEM((heads, send_rows, width), BF)]
        + ([pltpu.VMEM((seqs, pair, marks), BF)] if ring else []),
    )
    back = exchange(sent[:heads])
    out_shape = [shape_of((tokens_dev, features), BF)] * 4 + [shape_of((4, dh), F32)]
    if tiled:
        out_shape.append(shape_of((1, heads, dh, wide_part), F32))
    attended, dq, dk, dv, grad_norm, *tiles = call(
        functools.partial(unpack_kernel, heads=heads),
        out_shape,
        (head, *back),
        [SM] + [VM] * heads,
        "unpack",
        [pltpu.VMEM((heads, send_rows, width), BF)],
        keep=False,
    )
    if tiled:
        grad_proj = tiles[0]
    else:
        full = lax.all_gather(sent[-1], HEAD)
        inner = ("half", "part") if halves > 1 else "part"
        grad_proj = lax.psum_scatter(full, inner, scatter_dimension=2, tiled=True)[None] / parts
    return (attended, dq, dk, dv, grad_proj, grad_norm)


def solution(mesh):
    ctx, inner = mesh.shape["ctx"], mesh.shape["inner"]

    def whole(queries, keys, values, w_proj, ln_gain, ln_bias, cotangent):
        heads = w_proj.shape[0]
        part = min(heads, inner)
        sub = heads // part
        order = np.asarray(mesh.devices).reshape(ctx // sub, sub, inner // part, part)
        split = Mesh(order, ("seq", "sub", "half", "part"))
        every = P(("seq", "sub", "half", "part"), None)
        return jax.shard_map(
            per_device,
            mesh=split,
            in_specs=(every, every, every, P(), P(), P(), every),
            out_specs=(
                every,
                every,
                every,
                every,
                P(("seq", "sub"), None, None, ("half", "part")),
                P(),
            ),
            check_vma=False,
        )(queries, keys, values, w_proj, ln_gain, ln_bias, cotangent)

    return whole
```

```python
import functools
import math

import jax
import jax.numpy as jnp
import numpy as np
from jax import lax
from jax.experimental import pallas as pl
from jax.experimental.pallas import tpu as pltpu
from jax.sharding import Mesh
from jax.sharding import PartitionSpec as P


WIN = 128
EXTRA = 8
EPS = 1e-05
NEG = -1e30
BATCH = 8
VMEM_LIMIT = 24 * 1024 * 1024
BF = jnp.bfloat16
F32 = jnp.float32

NN = (((1,), (0,)), ((), ()))
NT = (((1,), (1,)), ((), ()))
SEQ = ("seq", "half")
HEAD = ("sub", "part")


def dot(a, b, dims=NN):
    return lax.dot_general(a, b, dims, preferred_element_type=F32)


def lanes(shape):
    return lax.broadcasted_iota(jnp.int32, shape, 1)


def rows(shape):
    return lax.broadcasted_iota(jnp.int32, shape, 0)


def peer_order():
    return [0, 7, 4, 2, 6, 5, 3, 1]


def gather_pieces(piece_refs, stack_ref, head):
    for k, ref in zip(peer_order(), piece_refs):
        stack_ref[head ^ k] = ref[...]


def scatter_pieces(stack_ref, piece_refs, head):
    for k, ref in zip(peer_order(), piece_refs):
        ref[...] = stack_ref[head ^ k]


def pack_kernel(head_ref, z_ref, q_ref, k_ref, v_ref, g_ref, w_src, gain_src, bias_src, *rest):
    *piece_refs, w_ref, gain_ref, bias_ref, stack_ref, buffer_ref, sems = rest
    del z_ref
    heads, _, width = stack_ref.shape
    dh = width // 4
    copies = []
    for slot, ref in enumerate((k_ref, v_ref, q_ref, g_ref)):
        copy = pltpu.make_async_copy(ref, buffer_ref.at[slot], sems.at[slot])
        copy.start()
        copies.append(copy)
    small = ((w_src.at[head_ref[0]], w_ref), (gain_src, gain_ref), (bias_src, bias_ref))
    extra = [
        pltpu.make_async_copy(src, dst, sems.at[len(copies) + slot])
        for slot, (src, dst) in enumerate(small)
    ]
    for copy in extra:
        copy.start()
    for slot, copy in enumerate(copies):
        copy.wait()
        for h in range(heads):
            stack_ref[h, :, slot * dh : (slot + 1) * dh] = buffer_ref[
                slot, :, h * dh : (h + 1) * dh
            ]
    scatter_pieces(stack_ref, piece_refs, head_ref[0])
    for copy in extra:
        copy.wait()


def split_rows(total_rows, width, pieces):
    r = rows((total_rows, width))
    out = jnp.zeros((total_rows, width), F32)
    for index, piece in enumerate(pieces):
        out = jnp.where(r == index, piece, out)
    return out.astype(BF)


def bf_pieces(x, count):
    out = []
    for _ in range(count):
        piece = x.astype(BF).astype(F32)
        out.append(piece)
        x = x - piece
    return out


def widen_proj(w):
    return jnp.concatenate([w, jnp.zeros_like(w)], axis=0)


def local_sums_kernel(head_ref, w_ref, *refs, heads):
    x_ref, expo_ref, mid_ref, *halo_refs = refs[heads:]
    gather_pieces(refs[:heads], x_ref, head_ref[0])
    _, tokens_dev, width = x_ref.shape
    count = heads * tokens_dev
    pair = width // 2
    kv = x_ref[:, :, :pair].reshape(count, pair)
    logits = dot(kv, widen_proj(w_ref[...]))
    peak = jnp.max(logits, axis=0, keepdims=True)
    expo = jnp.exp(logits - peak)
    total = jnp.sum(expo, axis=0, keepdims=True)
    expo_b = expo.astype(BF)
    expo_ref[...] = expo_b
    sums = dot(kv.T, expo_b).astype(BF)
    marks = sums.shape[1]
    tail = split_rows(EXTRA, marks, bf_pieces(peak, 3) + bf_pieces(total, 2))
    targets = [(mid_ref, None)]
    if halo_refs:
        targets += [(halo_refs[0], kv[count - WIN :]), (halo_refs[1], kv[:WIN])]
    for ref, halo in targets:
        ref[:pair, :marks] = sums
        ref[pair:, :marks] = tail
        if halo is not None:
            ref[:pair, marks:] = halo
            ref[pair:, marks:] = jnp.zeros((EXTRA, pair), BF)


def collect(own_ref, recv_refs, stack_ref, index, marks):
    count = len(recv_refs) + 1
    stack_ref[index] = own_ref[...]
    for shift, ref in enumerate(recv_refs, start=1):
        stack_ref[lax.rem(index + (count - shift), count)] = ref[:, :marks]


def as_column(ref):
    row = jnp.concatenate([ref[0:1, :], ref[1:2, :]], axis=1)
    size = row.shape[1]
    return jnp.sum(
        jnp.where(rows((size, size)) == lanes((size, size)), row, 0.0), axis=1, keepdims=True
    )


def spread(x, width):
    return jnp.concatenate([x] * (width // x.shape[1]), axis=1)


def row_max(x):
    return jnp.max(x, axis=1, keepdims=True)


def row_sum(x):
    return jnp.sum(x, axis=1, keepdims=True)


def window_forward_kernel(x_ref, gain_src, bias_src, early_ref, a_ref, at_ref, affine_ref, *, scale):
    count, width = x_ref.shape
    pair = width // 2
    dh = pair // 2
    segments = count // WIN
    low = lanes((WIN, pair)) < dh
    zero_b = jnp.zeros((WIN, pair), BF)
    for slot, src in enumerate((gain_src, bias_src)):
        affine_ref[slot * pair : (slot + 1) * pair] = jnp.broadcast_to(
            as_column(src), (pair, affine_ref.shape[1])
        )
    for s in range(segments):
        qg = x_ref[s * WIN : (s + 1) * WIN, pair:]
        q0 = jnp.where(low, (qg.astype(F32) * scale).astype(BF), zero_b)
        g0 = jnp.where(low, zero_b, qg)
        a = jnp.concatenate([q0, g0], axis=0)
        a_ref[2 * s * WIN : 2 * (s + 1) * WIN] = a
        at_ref[:, 2 * s * WIN : 2 * (s + 1) * WIN] = a.T
        kvw = x_ref[max(s - 1, 0) * WIN : min(s + 2, segments) * WIN, :pair]
        sw = dot(a, kvw, NT)
        scores, grads = sw[:WIN], sw[WIN:]
        top = row_max(scores)
        expo = jnp.exp(scores - top)
        expo_b = expo.astype(BF)
        out = dot(expo_b, kvw)
        part = row_sum(expo * grads)
        span = slice(s * WIN, (s + 1) * WIN)
        early_ref[span, :pair] = out
        for slot, stat in enumerate((top, row_sum(expo), part), start=1):
            early_ref[span, slot * pair : (slot + 1) * pair] = jnp.broadcast_to(stat, out.shape)


def landmark_forward_kernel(*refs, ring, seqs):
    lands = ring + 1 if ring else 3
    z_ref, early_ref, a_ref, at_ref = refs[:4]
    land_refs = refs[4 : 4 + lands]
    affine_ref = refs[4 + lands]
    outs = refs[5 + lands :]
    late_ref, rows_ref, mid_ref, plus_ref, minus_ref, stats_ref, *scratch = outs
    pair = mid_ref.shape[0]
    marks = mid_ref.shape[1]
    dh = pair // 2
    segments = early_ref.shape[0] // WIN
    z = z_ref[0]
    last = seqs - 1
    if ring:
        stack_ref = scratch[0]
        collect(land_refs[0], land_refs[1:], stack_ref, z, marks)
        halos = {0: land_refs[1][:pair, marks:], segments - 1: land_refs[-1][:pair, marks:]}
    else:
        stack_ref = land_refs[0]
        halos = {0: land_refs[1][...], segments - 1: land_refs[2][...]}
    groups = stack_ref.shape[0]

    peaks, totals = [], []
    for j in range(groups):
        tail = stack_ref[j, pair:, :].astype(F32)
        peaks.append(tail[0:1] + tail[1:2] + tail[2:3])
        totals.append(tail[3:4] + tail[4:5])
    peak = functools.reduce(jnp.maximum, peaks)
    total = jnp.zeros_like(peak)
    factors = [jnp.exp(p - peak) for p in peaks]
    for factor, part in zip(factors, totals):
        total = total + factor * part
    inv_total = 1.0 / total
    factors = [factor * inv_total for factor in factors]
    land_t, inverse = [], []
    for half in range(2):
        block = slice(half * dh, (half + 1) * dh)
        mean = factors[0] * stack_ref[0, block, :].astype(F32)
        for j in range(1, groups):
            mean = mean + factors[j] * stack_ref[j, block, :].astype(F32)
        stats_ref[pair + half * dh : pair + (half + 1) * dh] = mean
        centred = mean - jnp.mean(mean, axis=0, keepdims=True)
        inv = 1.0 / jnp.sqrt(jnp.mean(centred * centred, axis=0, keepdims=True) + EPS)
        normed = centred * inv
        stats_ref[block] = normed
        inverse.append(inv)
        gain = affine_ref[half * dh : (half + 1) * dh]
        bias = affine_ref[pair + half * dh : pair + (half + 1) * dh]
        land_t.append((normed * spread(gain, marks) + spread(bias, marks)).astype(BF))
    land_t = jnp.concatenate(land_t, axis=0)
    land = land_t.T
    own_tail = stack_ref[z, pair:, :].astype(F32)
    own_peak = own_tail[0:1] + own_tail[1:2] + own_tail[2:3]
    factor = jnp.exp(own_peak - peak) * inv_total
    r8 = rows((8, marks))
    stats_ref[2 * pair :] = jnp.where(r8 == 0, inverse[0], jnp.where(r8 == 1, inverse[1], factor))

    low = lanes((WIN, pair)) < dh
    land_grad = jnp.zeros((pair, marks), F32)
    halo_grads = {}
    for first in range(0, segments, BATCH):
        batch = range(first, min(first + BATCH, segments))
        spans = {s: slice(s * WIN, (s + 1) * WIN) for s in batch}
        blocks = {s: a_ref[2 * s * WIN : 2 * (s + 1) * WIN] for s in batch}
        early = {
            s: [early_ref[spans[s], slot * pair : (slot + 1) * pair] for slot in range(4)]
            for s in batch
        }
        sl = {s: dot(blocks[s], land_t) for s in batch}
        sh = {s: dot(blocks[s], halos[s], NT) for s in batch if s in halos}
        scores = {s: sl[s][:WIN] for s in batch}
        grads = {s: sl[s][WIN:] for s in batch}
        scores_h = {
            s: jnp.where(z == (0 if s == 0 else last), NEG, sh[s][:WIN]) for s in sh
        }
        top = {s: jnp.maximum(row_max(scores[s]), early[s][1]) for s in batch}
        for s in sh:
            top[s] = jnp.maximum(top[s], row_max(scores_h[s]))
        expo = {s: jnp.exp(scores[s] - spread(top[s], marks)) for s in batch}
        expo_h = {s: jnp.exp(scores_h[s] - top[s]) for s in sh}
        scale_e = {s: jnp.exp(early[s][1] - top[s]) for s in batch}
        total_row, part = {}, {}
        for s in batch:
            total_row[s] = row_sum(expo[s]) + early[s][2] * scale_e[s]
            part[s] = row_sum(expo[s] * grads[s]) + early[s][3] * scale_e[s]
            if s in sh:
                total_row[s] = total_row[s] + row_sum(expo_h[s])
                part[s] = part[s] + row_sum(expo_h[s] * sh[s][WIN:])
        inv = {s: 1.0 / total_row[s] for s in batch}
        delta = {s: part[s] * inv[s] for s in batch}
        b, b_h = {}, {}
        for s in batch:
            probs = expo[s] * spread(inv[s], marks)
            b[s] = jnp.concatenate(
                [(probs * (grads[s] - spread(delta[s], marks))).astype(BF), probs.astype(BF)],
                axis=0,
            )
            rows_ref[spans[s], :pair] = top[s] + jnp.log(total_row[s])
            rows_ref[spans[s], pair:] = delta[s]
        for s in sh:
            probs = expo_h[s] * inv[s]
            b_h[s] = jnp.concatenate(
                [(probs * (sh[s][WIN:] - delta[s])).astype(BF), probs.astype(BF)], axis=0
            )
        for s in batch:
            od = dot(b[s], land)
            if s in sh:
                od = od + dot(b_h[s], halos[s])
            late_ref[spans[s]] = jnp.where(
                low, od[:WIN], od[WIN:] + early[s][0] * (scale_e[s] * inv[s])
            )
        reach = slice(2 * batch[0] * WIN, 2 * (batch[-1] + 1) * WIN)
        land_grad = land_grad + dot(at_ref[:, reach], jnp.concatenate([b[s] for s in batch], axis=0))
        for s in sh:
            halo_grads[s] = dot(at_ref[:, 2 * s * WIN : 2 * (s + 1) * WIN], b_h[s]).astype(BF)
    land_b = land_grad.astype(BF)
    mid_ref[...] = land_b
    if ring:
        plus_ref[:, :marks] = land_b
        minus_ref[:, :marks] = land_b
        plus_ref[:, marks:] = halo_grads[segments - 1]
        minus_ref[:, marks:] = halo_grads[0]
    else:
        plus_ref[...] = halo_grads[segments - 1]
        minus_ref[...] = halo_grads[0]


def window_backward_kernel(x_ref, a_ref, at_ref, late_ref, rows_ref, od_ref, dkvt_ref, *, scale):
    count, width = x_ref.shape
    pair = width // 2
    dh = pair // 2
    segments = count // WIN
    dkvt_ref[...] = jnp.zeros(dkvt_ref.shape, F32)
    low = lanes((WIN, pair)) < dh
    for s in range(segments):
        span = slice(s * WIN, (s + 1) * WIN)
        near = slice(max(s - 1, 0) * WIN, min(s + 2, segments) * WIN)
        a = a_ref[2 * s * WIN : 2 * (s + 1) * WIN]
        kvw = x_ref[near, :pair]
        reach = near.stop - near.start
        sw = dot(a, kvw, NT)
        probs = jnp.exp(sw[:WIN] - spread(rows_ref[span, :pair], reach))
        grad_b = (probs * (sw[WIN:] - spread(rows_ref[span, pair:], reach))).astype(BF)
        late = late_ref[span]
        dq = (dot(grad_b, kvw) + late) * scale
        od_ref[span] = jnp.where(low, dq, late).astype(BF)
        b = jnp.concatenate([grad_b, probs.astype(BF)], axis=0)
        dkvt_ref[:, near] += dot(at_ref[:, 2 * s * WIN : 2 * (s + 1) * WIN], b)


def final_kernel(*refs, ring, seqs, heads, sub, parts, tiled):
    grads_in = ring + 1 if ring else 1
    z_ref, head_ref = refs[:2]
    grad_refs = refs[2 : 2 + grads_in]
    rest = refs[2 + grads_in :]
    if ring:
        prev_src, next_src = grad_refs[1], grad_refs[-1]
    else:
        prev_src, next_src, *rest = rest
    x_ref, w_ref, affine_ref, expo_ref, od_ref, dkvt_ref, stats_ref, *outs = rest
    count, width = x_ref.shape
    pair = width // 2
    dh = pair // 2
    marks = expo_ref.shape[1]
    if ring:
        stack_ref = outs.pop()
        collect(grad_refs[0], grad_refs[1:], stack_ref, z_ref[0], marks)
    else:
        stack_ref = grad_refs[0]
    send_ref = outs.pop()
    piece_refs, proj_refs = outs[:heads], outs[heads:]
    z = z_ref[0]
    from_prev = prev_src[:, prev_src.shape[1] - pair :].astype(F32)
    from_next = next_src[:, next_src.shape[1] - pair :].astype(F32)
    from_prev = jnp.where(z == 0, 0.0, from_prev)
    from_next = jnp.where(z == seqs - 1, 0.0, from_next)
    grad = stack_ref[0].astype(F32)
    for j in range(1, stack_ref.shape[0]):
        grad = grad + stack_ref[j].astype(F32)
    normed = stats_ref[:pair]
    mean = stats_ref[pair : 2 * pair]
    factor = stats_ref[2 * pair + 2 : 2 * pair + 3]
    gained = grad * spread(affine_ref[:pair], marks)
    blocks = []
    for half in range(2):
        part = slice(half * dh, (half + 1) * dh)
        g = gained[part]
        first = jnp.mean(g, axis=0, keepdims=True)
        second = jnp.mean(g * normed[part], axis=0, keepdims=True)
        inv = stats_ref[2 * pair + half : 2 * pair + half + 1]
        blocks.append(inv * (g - first - normed[part] * second))
    grad_mean = jnp.concatenate(blocks, axis=0)
    grad_b = grad_mean.astype(BF)
    column = jnp.sum(grad_b.astype(F32) * mean, axis=0, keepdims=True)
    scaled = (grad_mean * factor).astype(BF)

    gain_sum = jnp.sum(grad * normed, axis=1, keepdims=True)
    bias_sum = jnp.sum(grad, axis=1, keepdims=True)
    lane = lanes((pair, pair))
    square = jnp.where(lane == 0, gain_sum, jnp.where(lane == 1, bias_sum, 0.0)).T
    norm_hi = square[:8].astype(BF)
    norm_lo = (square[:8] - norm_hi.astype(F32)).astype(BF)
    norm_rows = jnp.concatenate(
        [
            jnp.concatenate([norm_hi, norm_lo], axis=1),
        ],
        axis=0,
    )

    kv = x_ref[:, :pair]
    wide = widen_proj(w_ref[...])
    expo_b = expo_ref[...]
    weights = expo_b.astype(F32) * factor
    grad_logit = (weights * (dot(kv, grad_b) - column)).astype(BF)
    land = dot(expo_b, scaled, NT) + dot(grad_logit, wide, NT)
    window = dkvt_ref[...].T
    dests, out_rows, _ = send_ref.shape
    step = count // dests
    dkv = land + window
    head_fix = from_prev.T
    tail_fix = from_next.T
    for d in range(dests):
        span = slice(d * step, (d + 1) * step)
        block = dkv[span]
        fix_top = head_fix if d == 0 else None
        fix_end = tail_fix if d == dests - 1 else None
        for at in range(0, step, WIN):
            piece = block[at : at + WIN]
            if fix_top is not None and at == 0:
                piece = piece + fix_top
            if fix_end is not None and at + WIN == step:
                piece = piece + fix_end
            send_ref[d, at : at + WIN, :pair] = piece.astype(BF)
        send_ref[d, :step, pair:] = od_ref[span]
        send_ref[d, out_rows - 8 :] = norm_rows
    kvt = kv.T
    group = count // sub
    for sb in range(sub):
        span = slice(sb * group, (sb + 1) * group)
        proj = dot(kvt[:, span], grad_logit[span])[:dh]
        if tiled:
            wide_part = marks // parts
            quarter = dh // 4
            for i in range(parts):
                tile = proj[:, i * wide_part : (i + 1) * wide_part].astype(BF)
                for k in range(4):
                    send_ref[
                        sb * parts + i, step : out_rows - 8, k * dh : (k + 1) * dh
                    ] = tile[k * quarter : (k + 1) * quarter]
        else:
            proj_refs[0][...] = proj
    scatter_pieces(send_ref, piece_refs, head_ref[0])


def unpack_kernel(head_ref, *refs, heads):
    att_ref, dq_ref, dk_ref, dv_ref, norm_ref, *proj_refs, r_ref = refs[heads:]
    gather_pieces(refs[:heads], r_ref, head_ref[0])
    heads, _, width = r_ref.shape
    dh = width // 4
    pair = 2 * dh
    step = att_ref.shape[0]
    for h in range(heads):
        cols = slice(h * dh, (h + 1) * dh)
        for slot, ref in enumerate((dk_ref, dv_ref, dq_ref, att_ref)):
            ref[:, cols] = r_ref[h, :step, slot * dh : (slot + 1) * dh]
    norm = jnp.zeros((8, pair), F32)
    for h in range(heads):
        block = r_ref[h, r_ref.shape[1] - 8 :, :].astype(F32)
        norm = norm + (block[:, :pair] + block[:, pair:])
    norm_ref[0:1] = norm[0:1, :dh]
    norm_ref[1:2] = norm[1:2, :dh]
    norm_ref[2:3] = norm[0:1, dh:]
    norm_ref[3:4] = norm[1:2, dh:]
    if proj_refs:
        proj_ref = proj_refs[0]
        quarter = dh // 4
        for h in range(heads):
            for k in range(4):
                proj_ref[0, h, k * quarter : (k + 1) * quarter] = r_ref[
                    h, step : r_ref.shape[1] - 8, k * dh : (k + 1) * dh
                ].astype(F32)


def shape_of(shape, dtype):
    return jax.ShapeDtypeStruct(shape, dtype)


VM = pl.BlockSpec(memory_space=pltpu.VMEM)
SM = pl.BlockSpec(memory_space=pltpu.SMEM)
ANY = pl.BlockSpec(memory_space=pltpu.HBM)


def call(kernel, out_shape, args, specs, scratch=(), keep=True, flops=0):
    args = [
        arg if spec is SM else pltpu.with_memory_space_constraint(arg, spec.memory_space)
        for arg, spec in zip(args, specs)
    ]
    if keep:
        out_shape = jax.tree.map(lambda s: pltpu.VMEM(s.shape, s.dtype), out_shape)
    cost = pl.CostEstimate(flops=flops, bytes_accessed=0, transcendentals=0) if flops else None
    return pl.pallas_call(
        kernel,
        out_shape=out_shape,
        in_specs=specs,
        out_specs=jax.tree.map(lambda _: VM, out_shape),
        scratch_shapes=scratch,
        compiler_params=pltpu.CompilerParams(vmem_limit_bytes=VMEM_LIMIT),
        cost_estimate=cost,
    )(*args)


def per_device(queries, keys, values, w_proj, ln_gain, ln_bias, cotangent):
    tokens_dev, features = queries.shape
    heads, dh, marks = w_proj.shape
    pair = 2 * dh
    width = 4 * dh
    count = tokens_dev * heads
    scale = 1.0 / math.sqrt(dh)
    seqs = lax.axis_size(SEQ)
    sub = lax.axis_size("sub")
    parts = lax.axis_size("part")
    halves = lax.axis_size("half")
    head = lax.axis_index(HEAD).astype(jnp.int32)
    z = lax.axis_index(SEQ).astype(jnp.int32)
    z = z.reshape(1)
    head = head.reshape(1)
    ring = seqs - 1 if 3 <= seqs <= 8 else 0
    wide_part = marks // parts
    tiled = halves == 1 and wide_part == dh and dh % 64 == 0

    def exchange(pieces):
        return [pieces[0]] + [
            lax.ppermute(piece, HEAD, [(i, i ^ k) for i in range(heads)])
            for k, piece in zip(peer_order()[1:], pieces[1:])
        ]

    *packed, w_head, gain, bias = call(
        pack_kernel,
        [shape_of((tokens_dev, width), BF)] * heads
        + [shape_of((dh, marks), BF)]
        + [shape_of((2, dh), F32)] * 2,
        (head, z, queries, keys, values, cotangent, w_proj, ln_gain, ln_bias),
        [SM] * 2 + [ANY] * 7,
        [
            pltpu.VMEM((heads, tokens_dev, width), BF),
            pltpu.VMEM((4, tokens_dev, features), BF),
            pltpu.SemaphoreType.DMA((7,)),
        ],
    )
    pieces = exchange(packed)

    rows_out = pair + EXTRA
    out_shape = [
        shape_of((heads, tokens_dev, width), BF),
        shape_of((count, marks), BF),
        shape_of((rows_out, marks), BF),
    ]
    if ring:
        out_shape += [shape_of((rows_out, marks + pair), BF)] * 2
    x, expo, mid, *halo_outs = call(
        functools.partial(local_sums_kernel, heads=heads),
        out_shape,
        (head, w_head, *pieces),
        [SM] + [VM] * (heads + 1),
    )
    x = x.reshape(count, width)

    def shifted(block, shift):
        return lax.ppermute(block, SEQ, [(i, (i + shift) % seqs) for i in range(seqs)])

    def forward(block, shift):
        route = [(i, i + shift) for i in range(seqs) if 0 <= i + shift < seqs]
        return lax.ppermute(block, SEQ, route)

    if ring:
        recv = [shifted(halo_outs[0], 1)]
        recv += [shifted(mid, k) for k in range(2, ring)]
        recv += [shifted(halo_outs[1], ring)]
        lands = [mid, *recv]
        halos = [recv[0], recv[-1]]
    else:
        halos = [forward(x[count - WIN :, :pair], 1), forward(x[:WIN, :pair], -1)]
        lands = [lax.all_gather(mid, SEQ), *halos]
    halo_wide = marks + pair if ring else pair
    work = 2 * count * 3 * WIN * pair
    early, a_all, at_all, affine = call(
        functools.partial(window_forward_kernel, scale=scale),
        [
            shape_of((count, 4 * pair), F32),
            shape_of((2 * count, pair), BF),
            shape_of((pair, 2 * count), BF),
            shape_of((2 * pair, pair), F32),
        ],
        (x, gain, bias),
        [VM] * 3,
        flops=3 * work,
    )
    late, row_stats, grad_mid, plus, minus, stats = call(
        functools.partial(landmark_forward_kernel, ring=ring, seqs=seqs),
        [
            shape_of((count, pair), F32),
            shape_of((count, 2 * pair), F32),
            shape_of((pair, marks), BF),
            shape_of((pair, halo_wide), BF),
            shape_of((pair, halo_wide), BF),
            shape_of((2 * pair + 8, marks), F32),
        ],
        (z, early, a_all, at_all, *lands, affine),
        [SM] + [VM] * (len(lands) + 4),
        [pltpu.VMEM((seqs, rows_out, marks), BF)] if ring else [],
    )
    if ring:
        grads = [grad_mid, shifted(plus, 1)]
        grads += [shifted(grad_mid, k) for k in range(2, ring)]
        grads += [shifted(minus, ring)]
    else:
        grads = [lax.all_gather(grad_mid, SEQ), forward(plus, 1), forward(minus, -1)]
    od, dkvt = call(
        functools.partial(window_backward_kernel, scale=scale),
        [shape_of((count, pair), BF), shape_of((pair, count), F32)],
        (x, a_all, at_all, late, row_stats),
        [VM] * 5,
        flops=5 * work,
    )
    send_rows = tokens_dev + 8 + (dh // 4 if tiled else 0)
    out_shape = [shape_of((send_rows, width), BF)] * heads
    if not tiled:
        out_shape.append(shape_of((dh, marks), F32))
    sent = call(
        functools.partial(
            final_kernel,
            ring=ring,
            seqs=seqs,
            heads=heads,
            sub=sub if tiled else 1,
            parts=parts,
            tiled=tiled,
        ),
        out_shape,
        (z, head, *grads, x, w_head, affine, expo, od, dkvt, stats),
        [SM, SM] + [VM] * (len(grads) + 7),
        [pltpu.VMEM((heads, send_rows, width), BF)]
        + ([pltpu.VMEM((seqs, pair, marks), BF)] if ring else []),
    )
    back = exchange(sent[:heads])
    out_shape = [shape_of((tokens_dev, features), BF)] * 4 + [shape_of((4, dh), F32)]
    if tiled:
        out_shape.append(shape_of((1, heads, dh, wide_part), F32))
    attended, dq, dk, dv, grad_norm, *tiles = call(
        functools.partial(unpack_kernel, heads=heads),
        out_shape,
        (head, *back),
        [SM] + [VM] * heads,
        [pltpu.VMEM((heads, send_rows, width), BF)],
        keep=False,
    )
    if tiled:
        grad_proj = tiles[0]
    else:
        full = lax.all_gather(sent[-1], HEAD)
        inner = ("half", "part") if halves > 1 else "part"
        grad_proj = lax.psum_scatter(full, inner, scatter_dimension=2, tiled=True)[None] / parts
    return (attended, dq, dk, dv, grad_proj, grad_norm)


def solution(mesh):
    ctx, inner = mesh.shape["ctx"], mesh.shape["inner"]

    def whole(queries, keys, values, w_proj, ln_gain, ln_bias, cotangent):
        heads = w_proj.shape[0]
        part = min(heads, inner)
        sub = heads // part
        order = np.asarray(mesh.devices).reshape(ctx // sub, sub, inner // part, part)
        split = Mesh(order, ("seq", "sub", "half", "part"))
        every = P(("seq", "sub", "half", "part"), None)
        step = jax.shard_map(
            per_device,
            mesh=split,
            in_specs=(every, every, every, P(), P(), P(), every),
            out_specs=(
                every,
                every,
                every,
                every,
                P(("seq", "sub"), None, None, ("half", "part")),
                P(),
            ),
            check_vma=False,
        )
        return step(queries, keys, values, w_proj, ln_gain, ln_bias, cotangent)

    return whole
```
